32 devices in a mesh: groups: 2 (over y), seq: 8 (over z, x), tp: 2 (over core).
Axes of the slice: x: 2, y: 2, z: 4, core: 2. Of those that a mesh axis runs over, the one named last changes fastest.
Arguments:
- stream: bfloat16 [128, 6144], P(('groups', 'seq'), 'tp'), parts along dimension 0, may hold values from -6 to 6
- queries: bfloat16 [128, 6144], P(('groups', 'seq'), 'tp'), parts along dimension 0, may hold values from -6 to 6
- key_rows: bfloat16 [128, 1024], P(('groups', 'seq'), 'tp'), parts along dimension 0, may hold values from -6 to 6
- value_rows: bfloat16 [128, 1024], P(('groups', 'seq'), 'tp'), parts along dimension 0, may hold values from -6 to 6
- routes: int32 [128, 2], P(('groups', 'seq')), parts along dimension 0, may hold values from 0 to 3, all different within a row; in each aligned block of 8 rows (0 to 7, 8 to 15, ...) at most 4 rows name the same one
- seq_length: int32 [2], P('groups'), parts along dimension 0, may hold values from 16 to 64
- norm_gain: float32 [6144], P('tp'), may hold values from 0.25 to 1.75
- router: float32 [6144, 4], P('tp'), may hold values from -0.078125 to 0.078125
- w_up: bfloat16 [6144, 32768], P('tp', 'seq'), may hold values from -0.078125 to 0.078125
- w_down: bfloat16 [32768, 6144], P('seq', 'tp'), may hold values from -0.0625 to 0.0625
- final_gain: float32 [6144], P('tp'), may hold values from 0.25 to 1.75
- value_weight: float32 [6144], P('tp'), may hold values from -0.078125 to 0.078125
- value_bias: float32 [1], replicated, may hold values from -3 to 3
Outputs:
- layer_out: bfloat16 [128, 6144], P(('groups', 'seq'), 'tp'), parts along dimension 0
- values: float32 [128], P(('groups', 'seq')), parts along dimension 0
The draws below stay inside these ranges and needn't reach their ends.
There are 2 independent parts, one for each index of `groups`. The reference program is written for one: setup_inputs(seed, part) draws one part's arguments, and reference() takes and returns one part's arrays. A program takes and returns all parts, laid end to end along the dimension named above; an argument that names none is the same for every part. Nothing has to cross between parts.
Inputs may be any that keep to these rules, and one draw needn't show every extreme that they name: `routes`: each row names two different experts; among the rows on one device no expert is named more than 4 times, and some device's rows name some expert exactly 4 times.
All inputs are finite; a program needn't handle non-finite values.
Results may differ from the reference program's by a relative error of at most 0.01.
Values may be sent and summed in bfloat16 or wider, within the bound.
A program may use at most 128 MiB of HBM per device.

```python
import math
import jax
import jax.numpy as jnp
import numpy as np
from jax import lax

D = 6144
HQ = 48
KVH = 8
HD = 128
EXPERTS = 4
F = 8192
LEN_DEV = 8
LENGTH = 64
CAP = 4
N_SEQ = 8


def draw_queries(key, part):
    values = jnp.clip(1.5 * jax.random.normal(jax.random.fold_in(key, 11), (LENGTH, HQ * HD), jnp.float32), -6.0, 6.0)
    return values.astype(jnp.bfloat16)


def draw_key_rows(key, part):
    values = jnp.clip(jax.random.normal(jax.random.fold_in(key, 12), (LENGTH, KVH * HD), jnp.float32), -6.0, 6.0)
    return values.astype(jnp.bfloat16)


def block_scale(stream_key, shape, split, least, top_value):
    gain = 1.0
    for position, shards_of in split:
        heights = jax.random.uniform(jax.random.fold_in(jax.random.fold_in(stream_key, 6), position), (shards_of,), jnp.float32, least / len(split), top_value / len(split))
        gain = gain * jnp.repeat(jnp.exp(heights), shape[position] // shards_of).reshape((-1,) + (1,) * (len(shape) - 1 - position))
    return gain


def shared_out(rng, own, number, rows, count, top, reach, lean):
    sequence = jax.random.permutation(rng, count)
    heavy_load, ordinary = shares(count, rows * top, reach, lean, True), shares(count, rows * top, reach, lean, False)
    places = jnp.arange(count)

    def named(lengths, rotation):
        used = int((lengths > 0).sum())
        fixed = max(1, used // 4)
        passed = fixed + (places - fixed + rotation * (used - fixed)) % max(1, count - fixed)
        return jnp.zeros((count,), jnp.int32).at[sequence[jnp.where(places < fixed, places, passed)]].set(jnp.asarray(lengths, jnp.int32))

    lengths = jnp.where(number % 4 == 0, named(heavy_load, number // 4), named(ordinary, number - number // 4 - 1))
    mixed = jax.random.permutation(jax.random.fold_in(own, 3), count)
    giver, taker = mixed[0:count // 2 * 2:2], mixed[1:count // 2 * 2:2]
    slack = jnp.minimum(lengths[giver] - 1, reach - lengths[taker]) // 2
    slack = jnp.where((giver == sequence[0]) | (taker == sequence[0]) | (lengths[taker] == 0), 0, jnp.maximum(slack, 0))
    passed = jax.random.randint(jax.random.fold_in(own, 4), (count // 2,), 0, 1 << 20) % (slack + 1)
    lengths = lengths.at[giver].add(-passed).at[taker].add(passed)
    members = jnp.searchsorted(jnp.cumsum(lengths), jnp.arange(rows * top), side="right").astype(jnp.int32)
    grid = members.reshape(top, rows).T
    grid = grid[jax.random.permutation(jax.random.fold_in(own, 1), rows)]
    rotation = jax.random.randint(jax.random.fold_in(own, 2), (rows, 1), 0, top)
    return jnp.take_along_axis(grid, (jnp.arange(top)[None, :] + rotation) % top, axis=1)


def shares(count, total, most, lean, full):
    portions = [(1 << 20) // math.isqrt(grade ** lean) + 1 for grade in range(1, count + 1)]
    largest = most if full else min(most, max(-(-total // count), total * portions[0] // sum(portions)))
    least = 1 if total - largest >= count - 1 else 0
    counts, spare = [largest] + [least] * (count - 1), total - largest - least * (count - 1)
    while spare > 0:
        movable = [i for i in range(1, count) if counts[i] < largest] or [i for i in range(1, count) if counts[i] < most]
        mass, remaining = sum([portions[i] for i in movable]), spare
        for i in movable:
            addition = min(most - counts[i], max(1, remaining * portions[i] // mass), spare)
            counts[i] = counts[i] + addition
            spare = spare - addition
    return np.array(counts)


def noise(own_key, extent, width, most, shards=(), kind=jnp.bfloat16):
    drawn = width * jax.random.normal(own_key, extent, jnp.float32)
    if shards:
        drawn = drawn * block_scale(own_key, extent, shards, -0.22, 0.18)
    return jnp.clip(drawn, -most, most).astype(kind)


def setup_inputs(seed: int = 0, part: int = 0) -> dict:
    arg_keys = jax.random.split(jax.random.key(seed), 14)
    part_keys = jax.random.split(jax.random.fold_in(arg_keys[13], part), 14)
    stream = noise(part_keys[0], (LENGTH, D), 1.0, 6.0, ((0, 8), (1, 2)))
    queries = draw_queries(jax.random.fold_in(jax.random.fold_in(arg_keys[13], part), 71), part)
    key_rows = draw_key_rows(jax.random.fold_in(jax.random.fold_in(arg_keys[13], part), 71), part)
    value_rows = noise(part_keys[3], (LENGTH, KVH * HD), 1.0, 6.0, ((0, 8), (1, 2)))
    routes_keys = jax.random.split(jax.random.fold_in(part_keys[4], 1), LENGTH // LEN_DEV)
    routes_turns = jax.random.permutation(jax.random.fold_in(part_keys[4], 3), LENGTH // LEN_DEV)
    routes = jax.vmap(lambda own, number: shared_out(jax.random.fold_in(part_keys[4], 2), own, number, LEN_DEV, EXPERTS, 2, CAP, 2))(routes_keys, routes_turns).reshape((LENGTH, 2))
    seq_length = jax.random.randint(part_keys[5], (1,), LENGTH // 4, LENGTH + 1).astype(jnp.int32)
    norm_gain = jnp.clip(1.0 + 0.15 * jax.random.normal(arg_keys[6], (D,), jnp.float32), 0.25, 1.75)
    router = noise(arg_keys[7], (D, EXPERTS), D ** -0.5, 0.078125, ((0, 2),), jnp.float32)
    w_up = noise(arg_keys[8], (D, EXPERTS * F), D ** -0.5, 0.078125, ((0, 2), (1, 8)))
    w_down = noise(arg_keys[9], (EXPERTS * F, D), F ** -0.5, 0.0625, ((0, 8), (1, 2)))
    final_gain = jnp.clip(1.0 + 0.15 * jax.random.normal(arg_keys[10], (D,), jnp.float32), 0.25, 1.75)
    value_weight = noise(arg_keys[11], (D,), D ** -0.5, 0.078125, ((0, 2),), jnp.float32)
    value_bias = noise(arg_keys[12], (1,), 1.0, 3.0, (), jnp.float32)
    return dict(stream=stream, queries=queries, key_rows=key_rows, value_rows=value_rows, routes=routes, seq_length=seq_length, norm_gain=norm_gain, router=router, w_up=w_up, w_down=w_down, final_gain=final_gain, value_weight=value_weight, value_bias=value_bias)


eps = 1e-05

def attention(queries, key_rows, value_rows, seq_limit):
    per_group = HQ // KVH
    positions = jnp.arange(LENGTH, dtype=jnp.int32)
    allowed = (positions[None, :] <= positions[:, None]) & (positions[None, :] < seq_limit)
    q_heads = queries.reshape(LENGTH, KVH, per_group, HD).transpose(1, 2, 0, 3)
    k_heads = key_rows.reshape(LENGTH, KVH, HD).transpose(1, 0, 2)
    v_heads = value_rows.reshape(LENGTH, KVH, HD).transpose(1, 0, 2)

    def one_head(triple):
        q_one, k_one, v_one = triple
        scores = jnp.einsum('gqd,cd->gqc', q_one.astype(jnp.float32), k_one.astype(jnp.float32)) / math.sqrt(HD)
        scores = jnp.where(allowed, scores, -jnp.inf)
        top_score = lax.optimization_barrier(jnp.max(scores, axis=-1, keepdims=True))
        expo = jnp.where(allowed, jnp.exp(scores - top_score), 0.0)
        rounded = lax.optimization_barrier(expo.astype(jnp.bfloat16))
        numer = jnp.einsum('gqc,cd->gqd', rounded.astype(jnp.float32), v_one.astype(jnp.float32))
        return numer / lax.optimization_barrier(jnp.sum(expo, axis=-1))[..., None]
    heads = lax.map(one_head, (q_heads, k_heads, v_heads))
    return heads.transpose(2, 0, 1, 3).reshape(LENGTH, HQ * HD)

def reference(stream, queries, key_rows, value_rows, routes, seq_length, norm_gain, router, w_up, w_down, final_gain, value_weight, value_bias):
    seq_limit = seq_length[0]
    hidden = stream.astype(jnp.float32) + attention(queries, key_rows, value_rows, seq_limit)
    normed = hidden * lax.rsqrt(lax.optimization_barrier(jnp.mean(hidden * hidden, axis=1, keepdims=True)) + eps) * norm_gain
    normed_half = normed.astype(jnp.bfloat16)
    logits = jnp.dot(normed, router, precision=lax.Precision.HIGHEST)
    chosen = (routes[:, :, None] == jnp.arange(EXPERTS, dtype=jnp.int32)).astype(jnp.float32)
    picked = lax.optimization_barrier(jnp.sum(chosen * logits[:, None, :], axis=2))
    gates = jax.nn.sigmoid(picked - picked[:, ::-1])
    coeffs = lax.optimization_barrier(jnp.sum(chosen * gates[:, :, None], axis=1))
    owners = N_SEQ // EXPERTS
    block = F // owners
    mixed = jnp.zeros((LENGTH, D), jnp.float32)
    for expert in range(EXPERTS):
        up_proj = jnp.dot(normed_half, w_up[:, expert * F:(expert + 1) * F], preferred_element_type=jnp.float32)
        active = jax.nn.silu(up_proj).astype(jnp.bfloat16)
        down_rows = w_down[expert * F:(expert + 1) * F]

        def add_block(total, index):
            act_part = lax.dynamic_slice_in_dim(active, index * block, block, 1)
            weight_part = lax.dynamic_slice_in_dim(down_rows, index * block, block, 0)
            piece = jnp.dot(act_part, weight_part, preferred_element_type=jnp.float32).astype(jnp.bfloat16)
            return (total + lax.optimization_barrier(piece).astype(jnp.float32), None)
        expert_out, _ = lax.scan(add_block, jnp.zeros((LENGTH, D), jnp.float32), jnp.arange(owners, dtype=jnp.int32))
        mixed = mixed + coeffs[:, expert:expert + 1] * expert_out
    final = hidden + mixed
    mean_sq = lax.optimization_barrier(jnp.mean(final * final, axis=1))
    estimate = lax.optimization_barrier(jnp.sum(final * final_gain * value_weight, axis=1)) * lax.rsqrt(mean_sq + eps) + value_bias[0]
    positions = jnp.arange(LENGTH, dtype=jnp.int32)
    estimate = jnp.where(positions < seq_limit, estimate, 0.0)
    return (final.astype(jnp.bfloat16), estimate)
```

```python
import functools
import math

import jax
import jax.numpy as jnp
from jax import lax
from jax.experimental import pallas as pl
from jax.experimental.pallas import tpu as pltpu
from jax.sharding import PartitionSpec as P

HD = 128
LANES = 128
SUB = 8
ROW_LIMIT = 64
VMEM_BYTES = 66 * 1000 * 1000

eps = 1e-05
masked = -1e30
MESH = pl.DeviceIdType.MESH


def remote(src, dst, send_sem, recv_sem, device):
    return pltpu.make_async_remote_copy(
        src_ref=src,
        dst_ref=dst,
        send_sem=send_sem,
        recv_sem=recv_sem,
        device_id=device,
        device_id_type=MESH,
    )


def largest(size, most):
    return max(w for w in range(LANES, most + 1, LANES) if size % w == 0)


def block_of(index, size, count):
    block = jnp.zeros_like(index)
    for step in range(1, count):
        block = block + (index >= step * size).astype(jnp.int32)
    return block


def layer_kernel(
    n,
    experts,
    width,
    *refs,
):
    inputs, (out_ref, val_ref) = refs[:13], refs[13:15]
    places, scratch = refs[15:26], refs[26:]
    k_ref, v_ref, q_ref, stream_ref, routes_ref, len_ref = places[:6]
    gain_ref, router_ref, fgain_ref, vw_ref, bias_ref = places[6:]
    order = (2, 3, 1, 0, 4, 5, 6, 7, 10, 11, 12)
    wup_ref, wdn_ref = inputs[8], inputs[9]
    (
    wup_v,
    wdn_v,
    kbuf,
    vbuf,
    hid,
    xsend,
    xin,
    xtail_send,
    xtail,
    xall,
    uown,
    usend,
    uin,
    active,
    rsend,
    rin,
    small_send,
    small_in,
    sq_send,
    sq_in,
    wup_sem,
    wdn_sem,
    kv_ss,
    kv_rs,
    x_ss,
    x_rs,
    u_ss,
    u_rs,
    r_ss,
    r_rs,
    s_ss,
    s_rs,
    t_ss,
    t_rs,
    in_sem,
    ) = scratch
    group = lax.axis_index("groups")
    me = lax.axis_index("seq")
    core = lax.axis_index("tp")
    partner = (group, me, 1 - core)
    rows, half = stream_ref.shape
    cap = rows // 2
    owners = n // experts
    up_chunks, up_rows, units = wup_v.shape
    down_chunks, _, down_cols = wdn_v.shape
    part_units = usend.shape[2]
    parts = units // part_units
    kv_heads = k_ref.shape[1] // HD
    per_group = half // HD // kv_heads
    keys = n * rows

    def up_copy(c):
        span = pl.ds(pl.multiple_of(c * up_rows, LANES), up_rows)
        return pltpu.make_async_copy(wup_ref.at[span, :], wup_v.at[c], wup_sem.at[c])

    def down_copy(c):
        cols = pl.ds(pl.multiple_of(c * down_cols, LANES), down_cols)
        return pltpu.make_async_copy(wdn_ref.at[:, cols], wdn_v.at[c], wdn_sem.at[c])

    def peer(step):
        return (group, lax.rem(me + step, n), core)

    barrier = pltpu.get_barrier_semaphore()
    for step in range(1, n):
        pl.semaphore_signal(barrier, inc=1, device_id=peer(step), device_id_type=MESH)
    pl.semaphore_signal(barrier, inc=1, device_id=partner, device_id_type=MESH)
    fetches = [
        pltpu.make_async_copy(inputs[number], place, in_sem.at[spot])
        for spot, (number, place) in enumerate(zip(order, places))
    ]
    for copy in fetches:
        copy.start()
    for copy in fetches:
        copy.wait()
    for c in range(up_chunks):
        up_copy(c).start()
    for c in range(down_chunks):
        down_copy(c).start()
    pl.semaphore_wait(barrier, n)

    sends = []
    for step in range(1, n):
        for which, (own, buf) in enumerate(((k_ref, kbuf), (v_ref, vbuf))):
            copy = remote(own, buf.at[me], kv_ss.at[which, step], kv_rs.at[which, me], peer(step))
            copy.start()
            sends.append(copy)
    kbuf[me] = k_ref[...]
    vbuf[me] = v_ref[...]

    later = lax.broadcasted_iota(jnp.int32, (rows, rows), 0)
    sooner = lax.broadcasted_iota(jnp.int32, (rows, rows), 1)

    def upright(line):
        spread = jnp.where(later == sooner, line.astype(jnp.float32), 0.0)
        return jnp.sum(spread, axis=1, keepdims=True).astype(jnp.int32)

    route0 = upright(routes_ref[0:1, :])
    route1 = upright(routes_ref[1:2, :])
    lower = (sooner < later).astype(jnp.float32).astype(jnp.bfloat16)

    def slots(count, per_expert):
        place = lax.broadcasted_iota(jnp.int32, (rows, count * cap), 1)
        block = block_of(place, cap, count)
        expert = block_of(block, per_expert, experts)
        slot = (place - block * cap).astype(jnp.float32)
        hits = ((route0 == expert) | (route1 == expert)).astype(jnp.float32)
        rank = jnp.dot(lower, hits.astype(jnp.bfloat16), preferred_element_type=jnp.float32)
        return expert, rank == slot

    expert, at_slot = slots(experts, 1)
    placing = (((route0 == expert) | (route1 == expert)) & at_slot).astype(jnp.float32)
    expert_r, at_slot_r = slots(n, owners)
    fetch0 = ((route0 == expert_r) & at_slot_r).astype(jnp.float32)
    fetch1 = ((route1 == expert_r) & at_slot_r).astype(jnp.float32)
    fetch = jnp.concatenate([fetch0, fetch1], axis=0).astype(jnp.bfloat16)

    for step in range(1, n):
        sender = lax.rem(me + n - step, n)
        for which, (own, buf) in enumerate(((k_ref, kbuf), (v_ref, vbuf))):
            remote(
                own, buf.at[sender], kv_ss.at[which, step], kv_rs.at[which, sender], peer(step)
            ).wait_recv()

    inv_root = 1.0 / math.sqrt(HD)
    query_row = lax.broadcasted_iota(jnp.int32, (per_group, rows, keys), 1).reshape(
        per_group * rows, keys
    )
    key_pos = lax.broadcasted_iota(jnp.int32, (per_group * rows, keys), 1)
    allowed = (key_pos <= me * rows + query_row) & (key_pos < len_ref[0])
    for head in range(kv_heads):
        cols = slice(head * HD, (head + 1) * HD)
        k_head = kbuf[:, :, cols].astype(jnp.float32).reshape(keys, HD).astype(jnp.bfloat16)
        v_head = vbuf[:, :, cols].astype(jnp.float32).reshape(keys, HD).astype(jnp.bfloat16)
        base = head * per_group
        q_head = jnp.concatenate(
            [
                q_ref[:, (base + g) * HD : (base + g + 1) * HD].astype(jnp.float32)
                for g in range(per_group)
            ],
            axis=0,
        ).astype(jnp.bfloat16)
        scores = (
            lax.dot_general(
                q_head, k_head, (((1,), (1,)), ((), ())), preferred_element_type=jnp.float32
            )
            * inv_root
        )
        scores = jnp.where(allowed, scores, masked)
        top = jnp.max(scores, axis=-1, keepdims=True)
        weights = jnp.where(allowed, jnp.exp(scores - top), 0.0)
        total = jnp.sum(weights, axis=-1, keepdims=True)
        update = jnp.dot(weights.astype(jnp.bfloat16), v_head, preferred_element_type=jnp.float32)
        update = update / total
        for g in range(per_group):
            out_cols = slice((base + g) * HD, (base + g + 1) * HD)
            hid[:, out_cols] = (
                stream_ref[:, out_cols].astype(jnp.float32) + update[g * rows : (g + 1) * rows]
            )

    hidden = hid[...]
    gained = hidden * gain_ref[...]
    squares = jnp.sum(hidden * hidden, axis=1, keepdims=True)
    lane = lax.broadcasted_iota(jnp.int32, (rows, LANES), 1)

    high = squares.astype(jnp.bfloat16).astype(jnp.float32)
    tail = jnp.where(lane == 0, high, jnp.where(lane == 1, squares - high, 0.0))
    placed = placing.astype(jnp.bfloat16)

    def pack(values):
        return lax.dot_general(
            placed,
            values.astype(jnp.bfloat16),
            (((0,), (0,)), ((), ())),
            preferred_element_type=jnp.float32,
        )

    def dispatch(src_of, dst, send_sem_of, recv_sem):
        for step in range(1, n):
            to = lax.rem(me + step, n)
            copy = remote(
                src_of(to // owners), dst, send_sem_of(step), recv_sem, (group, to, core)
            )
            copy.start()
            sends.append(copy)

    for c in range(up_chunks):
        packed = pack(gained[:, c * up_rows : (c + 1) * up_rows])
        for e in range(experts):
            xsend[c, e] = packed[e * cap : (e + 1) * cap].astype(jnp.bfloat16)
        dispatch(
            lambda e: xsend.at[c, e], xin.at[c, me], lambda step: x_ss.at[c, step], x_rs.at[c, me]
        )
        xin[c, me] = xsend[c, me // owners]
    packed = pack(tail)
    for e in range(experts):
        xtail_send[e] = packed[e * cap : (e + 1) * cap].astype(jnp.bfloat16)
    dispatch(lambda e: xtail_send.at[e], xtail.at[me], lambda step: t_ss.at[step], t_rs.at[me])
    xtail[me] = xtail_send[me // owners]

    stats = jnp.where(lane == experts, squares, 0.0)
    for e in range(experts):
        part = jnp.sum(gained * router_ref[e : e + 1, :], axis=1, keepdims=True)
        stats = jnp.where(lane == e, part, stats)
    small_send[0] = stats
    stat_copy = remote(small_send.at[0], small_in.at[0], s_ss.at[0], s_rs.at[0], partner)
    stat_copy.start()
    sends.append(stat_copy)

    uown[...] = jnp.zeros_like(uown)

    def gather_rows(c):
        for step in range(1, n):
            sender = lax.rem(me + n - step, n)
            remote(
                xsend.at[0, 0], xin.at[c, sender], x_ss.at[c, step], x_rs.at[c, sender], peer(step)
            ).wait_recv()
        arrived = jnp.concatenate([xin[c, d].astype(jnp.float32) for d in range(n)], axis=0)
        xall[...] = arrived.astype(jnp.bfloat16)
        up_copy(c).wait()

    @pl.loop(0, up_chunks - 1)
    def _(c):
        gather_rows(c)
        uown[...] += jnp.dot(xall[...], wup_v[c], preferred_element_type=jnp.float32)

    def exchange(p):
        return remote(usend.at[p], uin.at[p], u_ss.at[p], u_rs.at[p], partner)

    gather_rows(up_chunks - 1)
    for p in range(parts):
        cols = slice(p * part_units, (p + 1) * part_units)
        part = uown[:, cols] + jnp.dot(
            xall[...], wup_v[up_chunks - 1, :, cols], preferred_element_type=jnp.float32
        )
        uown[:, cols] = part
        usend[p] = part.astype(jnp.bfloat16)
        exchange(p).start()
        if p == 0:
            for step in range(1, n):
                sender = lax.rem(me + n - step, n)
                remote(
                    xtail_send.at[0], xtail.at[sender], t_ss.at[step], t_rs.at[sender], peer(step)
                ).wait_recv()
            ends = jnp.concatenate([xtail[d].astype(jnp.float32) for d in range(n)], axis=0)
            sq_send[...] = jnp.broadcast_to(ends[:, 0:1] + ends[:, 1:2], sq_send.shape)
            sq_copy = remote(sq_send, sq_in, s_ss.at[1], s_rs.at[1], partner)
            sq_copy.start()
            sends.append(sq_copy)

    sq_copy.wait_recv()
    scale = lax.rsqrt((sq_send[...] + sq_in[...])[:, 0:1] / width + eps)

    def activate(p):
        exchange(p).wait()
        cols = slice(p * part_units, (p + 1) * part_units)
        up = (uown[:, cols] + uin[p].astype(jnp.float32)) * scale
        active[:, cols] = (up / (1.0 + jnp.exp(-up))).astype(jnp.bfloat16)

    def send_back(c, down):
        for d in range(n):
            rsend[c, d] = down[d * cap : (d + 1) * cap].astype(jnp.bfloat16)
        for step in range(1, n):
            to = lax.rem(me + step, n)
            copy = remote(
                rsend.at[c, to], rin.at[c, me], r_ss.at[c, step], r_rs.at[c, me], (group, to, core)
            )
            copy.start()
            sends.append(copy)
        rin[c, me] = rsend[c, me]

    down = None
    for p in range(parts):
        activate(p)
        if p == 0:
            down_copy(0).wait()
        span = slice(p * part_units, (p + 1) * part_units)
        term = jnp.dot(active[:, span], wdn_v[0, span], preferred_element_type=jnp.float32)
        down = term if down is None else down + term
    send_back(0, down)
    for c in range(1, down_chunks):
        down_copy(c).wait()
        send_back(c, jnp.dot(active[...], wdn_v[c], preferred_element_type=jnp.float32))

    stat_copy.wait_recv()
    both = small_send[0] + small_in[0]
    norm_scale = lax.rsqrt(both[:, experts : experts + 1] / width + eps)
    logits = both * norm_scale
    picked0 = jnp.sum(jnp.where(lane == route0, logits, 0.0), axis=1, keepdims=True)
    picked1 = jnp.sum(jnp.where(lane == route1, logits, 0.0), axis=1, keepdims=True)
    gate0 = 1.0 / (1.0 + jnp.exp(picked1 - picked0))
    gate1 = 1.0 / (1.0 + jnp.exp(picked0 - picked1))

    sq_part = jnp.zeros((rows, 1), jnp.float32)
    dot_part = jnp.zeros((rows, 1), jnp.float32)
    for c in range(down_chunks):
        for step in range(1, n):
            sender = lax.rem(me + n - step, n)
            remote(
                rsend.at[c, 0], rin.at[c, sender], r_ss.at[c, step], r_rs.at[c, sender], peer(step)
            ).wait_recv()
        pieces = jnp.concatenate([rin[c, d].astype(jnp.float32) for d in range(n)], axis=0)
        fetched = jnp.dot(fetch, pieces.astype(jnp.bfloat16), preferred_element_type=jnp.float32)
        cols = slice(c * down_cols, (c + 1) * down_cols)
        final = hid[:, cols] + (gate0 * fetched[:rows] + gate1 * fetched[rows:])
        out_ref[:, cols] = final.astype(jnp.bfloat16)
        sq_part = sq_part + jnp.sum(final * final, axis=1, keepdims=True)
        dot_part = dot_part + jnp.sum(
            final * (fgain_ref[:, cols] * vw_ref[:, cols]), axis=1, keepdims=True
        )
    small_send[1] = jnp.where(lane == 0, sq_part, jnp.where(lane == 1, dot_part, 0.0))
    last = remote(small_send.at[1], small_in.at[1], s_ss.at[2], s_rs.at[2], partner)
    last.start()
    sends.append(last)
    last.wait_recv()
    ends = small_send[1] + small_in[1]
    estimate = ends[:, 1:2] * lax.rsqrt(ends[:, 0:1] / width + eps) + bias_ref[0]
    place = me * rows + lax.broadcasted_iota(jnp.int32, (rows, 1), 0)
    estimate = jnp.where(place < len_ref[0], estimate, 0.0)
    val_ref[...] = jnp.sum(jnp.where(later == sooner, estimate, 0.0), axis=0, keepdims=True)
    for copy in sends:
        copy.wait_send()


def store_kernel(out_ref, val_ref, out_hbm, val_hbm, sem):
    copies = [
        pltpu.make_async_copy(out_ref, out_hbm, sem.at[0]),
        pltpu.make_async_copy(val_ref, val_hbm, sem.at[1]),
    ]
    for copy in copies:
        copy.start()
    for copy in copies:
        copy.wait()


def fused(
    stream,
    queries,
    key_rows,
    value_rows,
    routes,
    seq_length,
    norm_gain,
    router,
    w_up,
    w_down,
    final_gain,
    value_weight,
    value_bias,
):
    rows, half = stream.shape
    n = lax.axis_size("seq")
    experts = router.shape[1]
    hidden_units = w_up.shape[1]
    cap = rows // 2
    arrivals = n * cap
    up_rows = largest(half, 768)
    up_chunks = half // up_rows
    down_cols = largest(half, 1024)
    down_chunks = half // down_cols
    part_units = hidden_units // 2
    vmem = pl.BlockSpec(memory_space=pltpu.VMEM)
    hbm = pl.BlockSpec(memory_space=pltpu.HBM)
    raw = pl.BlockSpec(memory_space=pl.ANY)
    bf16, f32 = jnp.bfloat16, jnp.float32
    dma = pltpu.SemaphoreType.DMA
    out, values = pl.pallas_call(
        functools.partial(layer_kernel, n, experts, half * lax.axis_size("tp")),
        out_shape=(pltpu.VMEM((rows, half), bf16), pltpu.VMEM((1, rows), f32)),
        in_specs=[hbm] * 13,
        out_specs=(vmem, vmem),
        scratch_shapes=[
            pltpu.VMEM(key_rows.shape, bf16),
            pltpu.VMEM(key_rows.shape, bf16),
            pltpu.VMEM(stream.shape, bf16),
            pltpu.VMEM(stream.shape, bf16),
            pltpu.VMEM((2, rows), jnp.int32),
            pltpu.SMEM((1,), jnp.int32),
            pltpu.VMEM((1, half), f32),
            pltpu.VMEM((experts, half), f32),
            pltpu.VMEM((1, half), f32),
            pltpu.VMEM((1, half), f32),
            pltpu.SMEM((1,), f32),
            pltpu.VMEM((up_chunks, up_rows, hidden_units), bf16),
            pltpu.VMEM((down_chunks, hidden_units, down_cols), bf16),
            pltpu.VMEM((n, rows, key_rows.shape[1]), bf16),
            pltpu.VMEM((n, rows, key_rows.shape[1]), bf16),
            pltpu.VMEM((rows, half), f32),
            pltpu.VMEM((up_chunks, experts, cap, up_rows), bf16),
            pltpu.VMEM((up_chunks, n, cap, up_rows), bf16),
            pltpu.VMEM((experts, cap, LANES), bf16),
            pltpu.VMEM((n, cap, LANES), bf16),
            pltpu.VMEM((arrivals, up_rows), bf16),
            pltpu.VMEM((arrivals, hidden_units), f32),
            pltpu.VMEM((2, arrivals, part_units), bf16),
            pltpu.VMEM((2, arrivals, part_units), bf16),
            pltpu.VMEM((arrivals, hidden_units), bf16),
            pltpu.VMEM((down_chunks, n, cap, down_cols), bf16),
            pltpu.VMEM((down_chunks, n, cap, down_cols), bf16),
            pltpu.VMEM((2, rows, LANES), f32),
            pltpu.VMEM((2, rows, LANES), f32),
            pltpu.VMEM((arrivals, LANES), f32),
            pltpu.VMEM((arrivals, LANES), f32),
            dma((up_chunks,)),
            dma((down_chunks,)),
            dma((2, n)),
            dma((2, n)),
            dma((up_chunks, n)),
            dma((up_chunks, n)),
            dma((2,)),
            dma((2,)),
            dma((down_chunks, n)),
            dma((down_chunks, n)),
            dma((3,)),
            dma((3,)),
            dma((n,)),
            dma((n,)),
            dma((11,)),
        ],
        compiler_params=pltpu.CompilerParams(
            collective_id=0, has_side_effects=True, vmem_limit_bytes=VMEM_BYTES
        ),
        name="layer",
    )(
        stream,
        queries,
        key_rows,
        value_rows,
        routes.T,
        seq_length,
        norm_gain.reshape(1, half),
        router.T,
        w_up,
        w_down,
        final_gain.reshape(1, half),
        value_weight.reshape(1, half),
        value_bias,
    )
    out, values = pl.pallas_call(
        store_kernel,
        out_shape=(
            jax.ShapeDtypeStruct((rows, half), bf16),
            jax.ShapeDtypeStruct((1, rows), f32),
        ),
        in_specs=[raw, raw],
        out_specs=(hbm, hbm),
        scratch_shapes=[dma((2,))],
        name="store",
    )(
        pltpu.with_memory_space_constraint(out, pltpu.VMEM),
        pltpu.with_memory_space_constraint(values, pltpu.VMEM),
    )
    return out, values.reshape(rows)


def unfused(
    stream,
    queries,
    key_rows,
    value_rows,
    routes,
    seq_length,
    norm_gain,
    router,
    w_up,
    w_down,
    final_gain,
    value_weight,
    value_bias,
):
    row_count = stream.shape[0]
    half_width = stream.shape[1]
    width = half_width * lax.axis_size("tp")
    experts = router.shape[1]
    seq_devices = lax.axis_size("seq")
    owners = seq_devices // experts
    my_index = lax.axis_index("seq")
    seq_limit = seq_length[0]
    positions = my_index * row_count + jnp.arange(row_count, dtype=jnp.int32)
    kv_heads = key_rows.shape[1] // HD
    per_group = queries.shape[1] // HD // kv_heads
    grouped = queries.reshape(row_count, kv_heads, per_group, HD)
    inv_root = 1.0 / math.sqrt(HD)
    slot_cap = row_count // 2
    run_max = jnp.full((kv_heads, per_group, row_count), masked, jnp.float32)
    key_block = lax.all_gather(key_rows, "seq", axis=0, tiled=True)
    value_block = lax.all_gather(value_rows, "seq", axis=0, tiled=True)
    key_count = key_block.shape[0]
    scores = (
        jnp.einsum(
            "qkgd,ckd->kgqc",
            grouped,
            key_block.reshape(key_count, kv_heads, HD),
            preferred_element_type=jnp.float32,
        )
        * inv_root
    )
    key_pos = jnp.arange(key_count, dtype=jnp.int32)
    allowed = (key_pos[None, :] <= positions[:, None]) & (key_pos[None, :] < seq_limit)
    scores = jnp.where(allowed, scores, masked)
    new_max = jnp.maximum(run_max, jnp.max(scores, axis=-1))
    weights = jnp.where(allowed, jnp.exp(scores - new_max[..., None]), 0.0)
    new_sum = jnp.sum(weights, axis=-1)
    update = jnp.einsum(
        "kgqc,ckd->kgqd",
        weights.astype(jnp.bfloat16),
        value_block.reshape(key_count, kv_heads, HD),
        preferred_element_type=jnp.float32,
    )
    attended = (update / new_sum[..., None]).transpose(2, 0, 1, 3).reshape(row_count, half_width)
    hidden = stream.astype(jnp.float32) + attended
    gained = hidden * norm_gain
    squares = jnp.sum(hidden * hidden, axis=1)
    total_sq = lax.psum(squares, "tp")
    norm_scale = lax.rsqrt(total_sq / width + eps)
    normed = gained * norm_scale[:, None]
    logits = lax.psum(jnp.dot(normed, router, precision=lax.Precision.HIGHEST), "tp")
    normed_half = normed.astype(jnp.bfloat16)
    expert_ids = jnp.arange(experts, dtype=jnp.int32)
    chosen = (routes[:, :, None] == expert_ids).astype(jnp.float32)
    picked = jnp.sum(chosen * logits[:, None, :], axis=2)
    gates = jax.nn.sigmoid(picked - picked[:, ::-1])
    flat_hits = chosen.reshape(row_count * 2, experts)
    earlier = jnp.cumsum(flat_hits, axis=0) - flat_hits
    slot_index = jnp.sum(earlier * flat_hits, axis=1).astype(jnp.int32)
    target = routes.reshape(row_count * 2) * slot_cap + slot_index
    placing = (target[:, None] == jnp.arange(experts * slot_cap, dtype=jnp.int32)[None, :]).astype(
        jnp.bfloat16
    )
    doubled = jnp.repeat(normed_half, 2, axis=0)
    packed = jnp.einsum("pe,pd->ed", placing, doubled, preferred_element_type=jnp.float32).astype(
        jnp.bfloat16
    )
    outgoing = jnp.broadcast_to(
        packed.reshape(experts, 1, slot_cap, half_width), (experts, owners, slot_cap, half_width)
    ).reshape(seq_devices, slot_cap, half_width)
    arrived = lax.all_to_all(outgoing, "seq", split_axis=0, concat_axis=0, tiled=True)
    lead = arrived.shape[0]
    items = arrived.shape[1]
    flat_rows = arrived.reshape(lead * items, half_width)
    up_part = jnp.dot(flat_rows, w_up, preferred_element_type=jnp.float32)
    up_total = lax.psum(up_part.astype(jnp.bfloat16), "tp").astype(jnp.float32)
    active = jax.nn.silu(up_total).astype(jnp.bfloat16)
    down_part = jnp.dot(active, w_down, preferred_element_type=jnp.float32).astype(jnp.bfloat16)
    partial_out = down_part.reshape(lead, items, half_width)
    returned = lax.all_to_all(partial_out, "seq", split_axis=0, concat_axis=0, tiled=True)
    summed = jnp.sum(
        returned.reshape(experts, owners, slot_cap, half_width), axis=1, dtype=jnp.float32
    ).reshape(experts * slot_cap, half_width)
    fetched = jnp.dot(placing.astype(jnp.float32), summed, precision=lax.Precision.HIGHEST)
    mixed = jnp.sum(fetched.reshape(row_count, 2, half_width) * gates[:, :, None], axis=1)
    final = hidden + mixed
    sq_part = jnp.sum(final * final, axis=1)
    dot_part = jnp.sum(final * (final_gain * value_weight), axis=1)
    sq_total, dot_total = lax.psum((sq_part, dot_part), "tp")
    estimate = dot_total * lax.rsqrt(sq_total / width + eps) + value_bias[0]
    estimate = jnp.where(positions < seq_limit, estimate, 0.0)
    return (final.astype(jnp.bfloat16), estimate)


def on_device(*args):
    stream, w_up = args[0], args[8]
    arrivals = lax.axis_size("seq") * (stream.shape[0] // 2)
    weight_bytes = 4 * w_up.shape[0] * w_up.shape[1]
    small = arrivals <= ROW_LIMIT and weight_bytes <= 52 * 1024 * 1024
    return fused(*args) if small else unfused(*args)


def solution(mesh):
    return jax.shard_map(
        on_device,
        mesh=mesh,
        in_specs=(
            P(("groups", "seq"), "tp"),
            P(("groups", "seq"), "tp"),
            P(("groups", "seq"), "tp"),
            P(("groups", "seq"), "tp"),
            P(("groups", "seq"), None),
            P("groups"),
            P("tp"),
            P("tp", None),
            P("tp", "seq"),
            P("seq", "tp"),
            P("tp"),
            P("tp"),
            P(),
        ),
        out_specs=(P(("groups", "seq"), "tp"), P(("groups", "seq"))),
        check_vma=False,
    )
```

```python
import functools
import math

import jax
import jax.numpy as jnp
from jax import lax
from jax.experimental import pallas as pl
from jax.experimental.pallas import tpu as pltpu
from jax.sharding import PartitionSpec as P

HD = 128
LANES = 128
SUB = 8
ROW_LIMIT = 64
VMEM_BYTES = 66 * 1000 * 1000

eps = 1e-05
masked = -1e30
MESH = pl.DeviceIdType.MESH


def remote(src, dst, send_sem, recv_sem, device):
    return pltpu.make_async_remote_copy(
        src_ref=src,
        dst_ref=dst,
        send_sem=send_sem,
        recv_sem=recv_sem,
        device_id=device,
        device_id_type=MESH,
    )


def largest(size, most):
    return max(w for w in range(LANES, most + 1, LANES) if size % w == 0)


def block_of(index, size, count):
    block = jnp.zeros_like(index)
    for step in range(1, count):
        block = block + (index >= step * size).astype(jnp.int32)
    return block


def layer_kernel(
    n,
    experts,
    width,
    *refs,
):
    inputs, (out_ref, val_ref) = refs[:13], refs[13:15]
    places, scratch = refs[15:24], refs[24:]
    q_ref, stream_ref, routes_ref, len_ref = places[:4]
    gain_ref, router_ref, fgain_ref, vw_ref, bias_ref = places[4:]
    order = (1, 0, 4, 5, 6, 7, 10, 11, 12)
    wup_ref, wdn_ref = inputs[8], inputs[9]
    (
    wup_v,
    wdn_v,
    kvbuf,
    hid,
    xsend,
    xin,
    xtail_send,
    xtail,
    xall,
    uown,
    usend,
    uin,
    active,
    rsend,
    rin,
    small_send,
    small_in,
    sq_send,
    sq_in,
    wup_sem,
    wdn_sem,
    kv_ss,
    kv_rs,
    x_ss,
    x_rs,
    u_ss,
    u_rs,
    r_ss,
    r_rs,
    s_ss,
    s_rs,
    t_ss,
    t_rs,
    in_sem,
    ) = scratch
    group = lax.axis_index("groups")
    me = lax.axis_index("seq")
    core = lax.axis_index("tp")
    partner = (group, me, 1 - core)
    rows, half = stream_ref.shape
    cap = rows // 2
    owners = n // experts
    up_chunks, up_rows, units = wup_v.shape
    down_chunks, _, down_cols = wdn_v.shape
    parts, _, part_units = usend.shape
    kv_heads = kvbuf.shape[3] // HD
    per_group = half // HD // kv_heads
    keys = n * rows
    others = pl.ds(0, n - 1)

    def up_copy(c):
        span = pl.ds(pl.multiple_of(c * up_rows, LANES), up_rows)
        return pltpu.make_async_copy(wup_ref.at[span, :], wup_v.at[c], wup_sem.at[c])

    def down_copy(c):
        cols = pl.ds(pl.multiple_of(c * down_cols, LANES), down_cols)
        return pltpu.make_async_copy(wdn_ref.at[:, cols], wdn_v.at[c], wdn_sem.at[c])

    def other(step):
        return step + (step >= me).astype(jnp.int32)

    kvbuf[...] = jnp.zeros_like(kvbuf)
    barrier = pltpu.get_barrier_semaphore()
    for step in range(n - 1):
        pl.semaphore_signal(
            barrier, inc=1, device_id=(group, other(step), core), device_id_type=MESH
        )
    pl.semaphore_signal(barrier, inc=1, device_id=partner, device_id_type=MESH)
    fetches = [
        pltpu.make_async_copy(inputs[2 + which], kvbuf.at[me, which], in_sem.at[which])
        for which in range(2)
    ] + [
        pltpu.make_async_copy(inputs[number], place, in_sem.at[2 + spot])
        for spot, (number, place) in enumerate(zip(order, places))
    ]
    for copy in fetches:
        copy.start()
    for copy in fetches:
        copy.wait()
    for c in range(up_chunks):
        up_copy(c).start()
    pl.semaphore_wait(barrier, n)

    def kv_copy(block, step, to):
        return remote(
            kvbuf.at[block], kvbuf.at[block], kv_ss.at[step], kv_rs.at[block], (group, to, core)
        )

    for step in range(n - 1, 0, -1):

        @pl.when(me + step < n)
        def _(step=step):
            kv_copy(me, step, lax.rem(me + step, n)).start()

    later = lax.broadcasted_iota(jnp.int32, (rows, rows), 0)
    sooner = lax.broadcasted_iota(jnp.int32, (rows, rows), 1)

    def upright(line):
        spread = jnp.where(later == sooner, line.astype(jnp.float32), 0.0)
        return jnp.sum(spread, axis=1, keepdims=True).astype(jnp.int32)

    route0 = upright(routes_ref[0:1, :])
    route1 = upright(routes_ref[1:2, :])
    lower = (sooner < later).astype(jnp.float32).astype(jnp.bfloat16)

    def slots(count, per_expert):
        place = lax.broadcasted_iota(jnp.int32, (rows, count * cap), 1)
        block = block_of(place, cap, count)
        expert = block_of(block, per_expert, experts)
        slot = (place - block * cap).astype(jnp.float32)
        hits = ((route0 == expert) | (route1 == expert)).astype(jnp.float32)
        rank = jnp.dot(lower, hits.astype(jnp.bfloat16), preferred_element_type=jnp.float32)
        return expert, rank == slot

    expert, at_slot = slots(experts, 1)
    placing = (((route0 == expert) | (route1 == expert)) & at_slot).astype(jnp.float32)
    placed = placing.astype(jnp.bfloat16)
    expert_r, at_slot_r = slots(n, owners)
    fetch0 = ((route0 == expert_r) & at_slot_r).astype(jnp.float32)
    fetch1 = ((route1 == expert_r) & at_slot_r).astype(jnp.float32)
    fetch = jnp.concatenate([fetch0, fetch1], axis=0).astype(jnp.bfloat16)

    for step in range(n - 1, 0, -1):

        @pl.when(step <= me)
        def _(step=step):
            kv_copy(lax.rem(me + n - step, n), step, me).wait_recv()

    for c in range(down_chunks):
        down_copy(c).start()

    def pack(values):
        return lax.dot_general(
            placed,
            values.astype(jnp.bfloat16),
            (((0,), (0,)), ((), ())),
            preferred_element_type=jnp.float32,
        )

    def dispatch(src_of, dst, send_sem, recv_sem):
        for step in range(n - 1):
            to = other(step)
            remote(src_of(to // owners), dst, send_sem, recv_sem, (group, to, core)).start()

    inv_root = 1.0 / math.sqrt(HD)
    query_row = lax.broadcasted_iota(jnp.int32, (per_group, rows, keys), 1).reshape(
        per_group * rows, keys
    )
    key_pos = lax.broadcasted_iota(jnp.int32, (per_group * rows, keys), 1)
    allowed = (key_pos <= me * rows + query_row) & (key_pos < len_ref[0])
    all_scores = []
    for head in range(kv_heads):
        cols = slice(head * HD, (head + 1) * HD)
        k_head = kvbuf[:, 0, :, cols].astype(jnp.float32).reshape(keys, HD).astype(jnp.bfloat16)
        base = head * per_group
        q_head = jnp.concatenate(
            [
                q_ref[:, (base + g) * HD : (base + g + 1) * HD].astype(jnp.float32)
                for g in range(per_group)
            ],
            axis=0,
        ).astype(jnp.bfloat16)
        all_scores.append(
            lax.dot_general(
                q_head, k_head, (((1,), (1,)), ((), ())), preferred_element_type=jnp.float32
            )
            * inv_root
        )
    updates = []
    for head in range(kv_heads):
        cols = slice(head * HD, (head + 1) * HD)
        v_head = kvbuf[:, 1, :, cols].astype(jnp.float32).reshape(keys, HD).astype(jnp.bfloat16)
        scores = jnp.where(allowed, all_scores[head], masked)
        top = jnp.max(scores, axis=-1, keepdims=True)
        weights = jnp.where(allowed, jnp.exp(scores - top), 0.0)
        total = jnp.sum(weights, axis=-1, keepdims=True)
        update = jnp.dot(weights.astype(jnp.bfloat16), v_head, preferred_element_type=jnp.float32)
        updates.append(update / total)
    squares = jnp.zeros((rows, 1), jnp.float32)
    chunks = []
    for c in range(up_chunks):
        span = slice(c * up_rows, (c + 1) * up_rows)
        update = jnp.concatenate(
            [updates[c][g * rows : (g + 1) * rows] for g in range(per_group)], axis=1
        )
        hidden = stream_ref[:, span].astype(jnp.float32) + update
        hid[:, span] = hidden
        gained = hidden * gain_ref[:, span]
        chunks.append(gained)
        squares = squares + jnp.sum(hidden * hidden, axis=1, keepdims=True)
        packed = pack(gained)
        for e in range(experts):
            xsend[c, e] = packed[e * cap : (e + 1) * cap].astype(jnp.bfloat16)
        dispatch(lambda e: xsend.at[c, e], xin.at[c, me], x_ss.at[0], x_rs.at[c])
        xin[c, me] = xsend[c, me // owners]
    lane = lax.broadcasted_iota(jnp.int32, (rows, LANES), 1)
    high = squares.astype(jnp.bfloat16).astype(jnp.float32)
    tail = jnp.where(lane == 0, high, jnp.where(lane == 1, squares - high, 0.0))
    packed = pack(tail)
    for e in range(experts):
        xtail_send[e] = packed[e * cap : (e + 1) * cap].astype(jnp.bfloat16)
    dispatch(lambda e: xtail_send.at[e], xtail.at[me], t_ss.at[0], t_rs.at[0])
    xtail[me] = xtail_send[me // owners]

    stats = jnp.where(lane == experts, squares, 0.0)
    for e in range(experts):
        part = jnp.zeros((rows, 1), jnp.float32)
        for c in range(up_chunks):
            weight = router_ref[e : e + 1, c * up_rows : (c + 1) * up_rows]
            part = part + jnp.sum(chunks[c] * weight, axis=1, keepdims=True)
        stats = jnp.where(lane == e, part, stats)
    small_send[0] = stats
    stat_copy = remote(small_send.at[0], small_in.at[0], s_ss.at[0], s_rs.at[0], partner)
    stat_copy.start()

    def arrival(block, recv_sem):
        return remote(block, block, x_ss.at[0], recv_sem, partner)

    def gather_rows(c):
        arrival(xin.at[c, others], x_rs.at[c]).wait_recv()
        arrived = jnp.concatenate([xin[c, d].astype(jnp.float32) for d in range(n)], axis=0)
        up_copy(c).wait()
        return arrived.astype(jnp.bfloat16)

    def exchange(p):
        return remote(usend.at[p], uin.at[p], u_ss.at[p], u_rs.at[p], partner)

    for c in range(up_chunks - 1):
        xall[...] = gather_rows(c)
        term = jnp.dot(xall[...], wup_v[c], preferred_element_type=jnp.float32)
        uown[...] = term if c == 0 else uown[...] + term

    xall[...] = gather_rows(up_chunks - 1)
    arrival(xtail.at[others], t_rs.at[0]).wait_recv()
    ends = jnp.concatenate([xtail[d].astype(jnp.float32) for d in range(n)], axis=0)
    sq_send[...] = jnp.broadcast_to(ends[:, 0:1] + ends[:, 1:2], sq_send.shape)
    sq_copy = remote(sq_send, sq_in, s_ss.at[1], s_rs.at[1], partner)
    sq_copy.start()
    for p in range(parts):
        cols = slice(p * part_units, (p + 1) * part_units)
        part = uown[:, cols] + jnp.dot(
            xall[...], wup_v[up_chunks - 1, :, cols], preferred_element_type=jnp.float32
        )
        uown[:, cols] = part
        usend[p] = part.astype(jnp.bfloat16)
        exchange(p).start()

    sq_copy.wait_recv()
    scale = lax.rsqrt((sq_send[...] + sq_in[...])[:, 0:1] / width + eps)

    def activate(p):
        exchange(p).wait_recv()
        cols = slice(p * part_units, (p + 1) * part_units)
        up = (uown[:, cols] + uin[p].astype(jnp.float32)) * scale
        active[:, cols] = (up / (1.0 + jnp.exp(-up))).astype(jnp.bfloat16)

    def send_back(c, down):
        for d in range(n):
            rsend[c, d] = down[d * cap : (d + 1) * cap].astype(jnp.bfloat16)
        for step in range(n - 1):
            to = other(step)
            remote(
                rsend.at[c, to], rin.at[c, me], r_ss.at[0], r_rs.at[c], (group, to, core)
            ).start()
        rin[c, me] = rsend[c, me]

    first = min(2, down_chunks)
    downs = [None] * first
    for p in range(parts):
        activate(p)
        span = slice(p * part_units, (p + 1) * part_units)
        for c in range(first):
            if p == 0:
                down_copy(c).wait()
            term = jnp.dot(active[:, span], wdn_v[c, span], preferred_element_type=jnp.float32)
            downs[c] = term if p == 0 else downs[c] + term
    for c in range(first):
        send_back(c, downs[c])
    for c in range(first, down_chunks):
        down_copy(c).wait()
        send_back(c, jnp.dot(active[...], wdn_v[c], preferred_element_type=jnp.float32))

    stat_copy.wait_recv()
    both = small_send[0] + small_in[0]
    norm_scale = lax.rsqrt(both[:, experts : experts + 1] / width + eps)
    logits = both * norm_scale
    picked0 = jnp.sum(jnp.where(lane == route0, logits, 0.0), axis=1, keepdims=True)
    picked1 = jnp.sum(jnp.where(lane == route1, logits, 0.0), axis=1, keepdims=True)
    gate0 = 1.0 / (1.0 + jnp.exp(picked1 - picked0))
    gate1 = 1.0 / (1.0 + jnp.exp(picked0 - picked1))

    sq_part = jnp.zeros((rows, 1), jnp.float32)
    dot_part = jnp.zeros((rows, 1), jnp.float32)
    for c in range(down_chunks):
        arrival(rin.at[c, others], r_rs.at[c]).wait_recv()
        pieces = jnp.concatenate([rin[c, d].astype(jnp.float32) for d in range(n)], axis=0)
        fetched = jnp.dot(fetch, pieces.astype(jnp.bfloat16), preferred_element_type=jnp.float32)
        cols = slice(c * down_cols, (c + 1) * down_cols)
        final = hid[:, cols] + (gate0 * fetched[:rows] + gate1 * fetched[rows:])
        out_ref[:, cols] = final.astype(jnp.bfloat16)
        sq_part = sq_part + jnp.sum(final * final, axis=1, keepdims=True)
        dot_part = dot_part + jnp.sum(
            final * (fgain_ref[:, cols] * vw_ref[:, cols]), axis=1, keepdims=True
        )
    small_send[1] = jnp.where(lane == 0, sq_part, jnp.where(lane == 1, dot_part, 0.0))
    last = remote(small_send.at[1], small_in.at[1], s_ss.at[2], s_rs.at[2], partner)
    last.start()

    def sent(block, send_sem):
        remote(block, block, send_sem, r_rs.at[0], partner).wait_send()

    for step in range(1, n):

        @pl.when(me + step < n)
        def _(step=step):
            kv_copy(me, step, me).wait_send()

    sent(xin.at[:, others], x_ss.at[0])
    sent(xtail.at[others], t_ss.at[0])
    sent(rin.at[:, others], r_ss.at[0])
    for p in range(parts):
        exchange(p).wait_send()
    stat_copy.wait_send()
    sq_copy.wait_send()
    last.wait_recv()
    ends = small_send[1] + small_in[1]
    estimate = ends[:, 1:2] * lax.rsqrt(ends[:, 0:1] / width + eps) + bias_ref[0]
    place = me * rows + lax.broadcasted_iota(jnp.int32, (rows, 1), 0)
    estimate = jnp.where(place < len_ref[0], estimate, 0.0)
    val_ref[...] = jnp.sum(jnp.where(later == sooner, estimate, 0.0), axis=0, keepdims=True)
    last.wait_send()


def store_kernel(out_ref, val_ref, out_hbm, val_hbm, sem):
    copies = [
        pltpu.make_async_copy(out_ref, out_hbm, sem.at[0]),
        pltpu.make_async_copy(val_ref, val_hbm, sem.at[1]),
    ]
    for copy in copies:
        copy.start()
    for copy in copies:
        copy.wait()


def fused(
    stream,
    queries,
    key_rows,
    value_rows,
    routes,
    seq_length,
    norm_gain,
    router,
    w_up,
    w_down,
    final_gain,
    value_weight,
    value_bias,
):
    rows, half = stream.shape
    n = lax.axis_size("seq")
    experts = router.shape[1]
    hidden_units = w_up.shape[1]
    cap = rows // 2
    arrivals = n * cap
    kv_cols = key_rows.shape[1]
    up_chunks = kv_cols // HD
    up_rows = half // up_chunks
    down_cols = largest(half, 512)
    down_chunks = half // down_cols
    parts = 4
    part_units = hidden_units // parts
    vmem = pl.BlockSpec(memory_space=pltpu.VMEM)
    hbm = pl.BlockSpec(memory_space=pltpu.HBM)
    raw = pl.BlockSpec(memory_space=pl.ANY)
    bf16, f32 = jnp.bfloat16, jnp.float32
    dma = pltpu.SemaphoreType.DMA
    out, values = pl.pallas_call(
        functools.partial(layer_kernel, n, experts, half * lax.axis_size("tp")),
        out_shape=(pltpu.VMEM((rows, half), bf16), pltpu.VMEM((1, rows), f32)),
        in_specs=[hbm] * 13,
        out_specs=(vmem, vmem),
        scratch_shapes=[
            pltpu.VMEM(stream.shape, bf16),
            pltpu.VMEM(stream.shape, bf16),
            pltpu.VMEM((2, rows), jnp.int32),
            pltpu.SMEM((1,), jnp.int32),
            pltpu.VMEM((1, half), f32),
            pltpu.VMEM((experts, half), f32),
            pltpu.VMEM((1, half), f32),
            pltpu.VMEM((1, half), f32),
            pltpu.SMEM((1,), f32),
            pltpu.VMEM((up_chunks, up_rows, hidden_units), bf16),
            pltpu.VMEM((down_chunks, hidden_units, down_cols), bf16),
            pltpu.VMEM((n, 2, rows, kv_cols), bf16),
            pltpu.VMEM((rows, half), f32),
            pltpu.VMEM((up_chunks, experts, cap, up_rows), bf16),
            pltpu.VMEM((up_chunks, n, cap, up_rows), bf16),
            pltpu.VMEM((experts, cap, LANES), bf16),
            pltpu.VMEM((n, cap, LANES), bf16),
            pltpu.VMEM((arrivals, up_rows), bf16),
            pltpu.VMEM((arrivals, hidden_units), f32),
            pltpu.VMEM((parts, arrivals, part_units), bf16),
            pltpu.VMEM((parts, arrivals, part_units), bf16),
            pltpu.VMEM((arrivals, hidden_units), bf16),
            pltpu.VMEM((down_chunks, n, cap, down_cols), bf16),
            pltpu.VMEM((down_chunks, n, cap, down_cols), bf16),
            pltpu.VMEM((2, rows, LANES), f32),
            pltpu.VMEM((2, rows, LANES), f32),
            pltpu.VMEM((arrivals, LANES), f32),
            pltpu.VMEM((arrivals, LANES), f32),
            dma((up_chunks,)),
            dma((down_chunks,)),
            dma((n,)),
            dma((n,)),
            dma((1,)),
            dma((up_chunks,)),
            dma((parts,)),
            dma((parts,)),
            dma((1,)),
            dma((down_chunks,)),
            dma((3,)),
            dma((3,)),
            dma((1,)),
            dma((1,)),
            dma((11,)),
        ],
        compiler_params=pltpu.CompilerParams(
            collective_id=0, has_side_effects=True, vmem_limit_bytes=VMEM_BYTES
        ),
        name="layer",
    )(
        stream,
        queries,
        key_rows,
        value_rows,
        routes.T,
        seq_length,
        norm_gain.reshape(1, half),
        router.T,
        w_up,
        w_down,
        final_gain.reshape(1, half),
        value_weight.reshape(1, half),
        value_bias,
    )
    out, values = pl.pallas_call(
        store_kernel,
        out_shape=(
            jax.ShapeDtypeStruct((rows, half), bf16),
            jax.ShapeDtypeStruct((1, rows), f32),
        ),
        in_specs=[raw, raw],
        out_specs=(hbm, hbm),
        scratch_shapes=[dma((2,))],
        name="store",
    )(
        pltpu.with_memory_space_constraint(out, pltpu.VMEM),
        pltpu.with_memory_space_constraint(values, pltpu.VMEM),
    )
    return out, values.reshape(rows)


def unfused(
    stream,
    queries,
    key_rows,
    value_rows,
    routes,
    seq_length,
    norm_gain,
    router,
    w_up,
    w_down,
    final_gain,
    value_weight,
    value_bias,
):
    row_count = stream.shape[0]
    half_width = stream.shape[1]
    width = half_width * lax.axis_size("tp")
    experts = router.shape[1]
    seq_devices = lax.axis_size("seq")
    owners = seq_devices // experts
    my_index = lax.axis_index("seq")
    seq_limit = seq_length[0]
    positions = my_index * row_count + jnp.arange(row_count, dtype=jnp.int32)
    kv_heads = key_rows.shape[1] // HD
    per_group = queries.shape[1] // HD // kv_heads
    grouped = queries.reshape(row_count, kv_heads, per_group, HD)
    inv_root = 1.0 / math.sqrt(HD)
    slot_cap = row_count // 2
    run_max = jnp.full((kv_heads, per_group, row_count), masked, jnp.float32)
    key_block = lax.all_gather(key_rows, "seq", axis=0, tiled=True)
    value_block = lax.all_gather(value_rows, "seq", axis=0, tiled=True)
    key_count = key_block.shape[0]
    scores = (
        jnp.einsum(
            "qkgd,ckd->kgqc",
            grouped,
            key_block.reshape(key_count, kv_heads, HD),
            preferred_element_type=jnp.float32,
        )
        * inv_root
    )
    key_pos = jnp.arange(key_count, dtype=jnp.int32)
    allowed = (key_pos[None, :] <= positions[:, None]) & (key_pos[None, :] < seq_limit)
    scores = jnp.where(allowed, scores, masked)
    new_max = jnp.maximum(run_max, jnp.max(scores, axis=-1))
    weights = jnp.where(allowed, jnp.exp(scores - new_max[..., None]), 0.0)
    new_sum = jnp.sum(weights, axis=-1)
    update = jnp.einsum(
        "kgqc,ckd->kgqd",
        weights.astype(jnp.bfloat16),
        value_block.reshape(key_count, kv_heads, HD),
        preferred_element_type=jnp.float32,
    )
    attended = (update / new_sum[..., None]).transpose(2, 0, 1, 3).reshape(row_count, half_width)
    hidden = stream.astype(jnp.float32) + attended
    gained = hidden * norm_gain
    squares = jnp.sum(hidden * hidden, axis=1)
    total_sq = lax.psum(squares, "tp")
    norm_scale = lax.rsqrt(total_sq / width + eps)
    normed = gained * norm_scale[:, None]
    logits = lax.psum(jnp.dot(normed, router, precision=lax.Precision.HIGHEST), "tp")
    normed_half = normed.astype(jnp.bfloat16)
    expert_ids = jnp.arange(experts, dtype=jnp.int32)
    chosen = (routes[:, :, None] == expert_ids).astype(jnp.float32)
    picked = jnp.sum(chosen * logits[:, None, :], axis=2)
    gates = jax.nn.sigmoid(picked - picked[:, ::-1])
    flat_hits = chosen.reshape(row_count * 2, experts)
    earlier = jnp.cumsum(flat_hits, axis=0) - flat_hits
    slot_index = jnp.sum(earlier * flat_hits, axis=1).astype(jnp.int32)
    target = routes.reshape(row_count * 2) * slot_cap + slot_index
    placing = (target[:, None] == jnp.arange(experts * slot_cap, dtype=jnp.int32)[None, :]).astype(
        jnp.bfloat16
    )
    doubled = jnp.repeat(normed_half, 2, axis=0)
    packed = jnp.einsum("pe,pd->ed", placing, doubled, preferred_element_type=jnp.float32).astype(
        jnp.bfloat16
    )
    outgoing = jnp.broadcast_to(
        packed.reshape(experts, 1, slot_cap, half_width), (experts, owners, slot_cap, half_width)
    ).reshape(seq_devices, slot_cap, half_width)
    arrived = lax.all_to_all(outgoing, "seq", split_axis=0, concat_axis=0, tiled=True)
    lead = arrived.shape[0]
    items = arrived.shape[1]
    flat_rows = arrived.reshape(lead * items, half_width)
    up_part = jnp.dot(flat_rows, w_up, preferred_element_type=jnp.float32)
    up_total = lax.psum(up_part.astype(jnp.bfloat16), "tp").astype(jnp.float32)
    active = jax.nn.silu(up_total).astype(jnp.bfloat16)
    down_part = jnp.dot(active, w_down, preferred_element_type=jnp.float32).astype(jnp.bfloat16)
    partial_out = down_part.reshape(lead, items, half_width)
    returned = lax.all_to_all(partial_out, "seq", split_axis=0, concat_axis=0, tiled=True)
    summed = jnp.sum(
        returned.reshape(experts, owners, slot_cap, half_width), axis=1, dtype=jnp.float32
    ).reshape(experts * slot_cap, half_width)
    fetched = jnp.dot(placing.astype(jnp.float32), summed, precision=lax.Precision.HIGHEST)
    mixed = jnp.sum(fetched.reshape(row_count, 2, half_width) * gates[:, :, None], axis=1)
    final = hidden + mixed
    sq_part = jnp.sum(final * final, axis=1)
    dot_part = jnp.sum(final * (final_gain * value_weight), axis=1)
    sq_total, dot_total = lax.psum((sq_part, dot_part), "tp")
    estimate = dot_total * lax.rsqrt(sq_total / width + eps) + value_bias[0]
    estimate = jnp.where(positions < seq_limit, estimate, 0.0)
    return (final.astype(jnp.bfloat16), estimate)


def on_device(*args):
    stream, w_up = args[0], args[8]
    arrivals = lax.axis_size("seq") * (stream.shape[0] // 2)
    weight_bytes = 4 * w_up.shape[0] * w_up.shape[1]
    small = arrivals <= ROW_LIMIT and weight_bytes <= 52 * 1024 * 1024
    return fused(*args) if small else unfused(*args)


def solution(mesh):
    return jax.shard_map(
        on_device,
        mesh=mesh,
        in_specs=(
            P(("groups", "seq"), "tp"),
            P(("groups", "seq"), "tp"),
            P(("groups", "seq"), "tp"),
            P(("groups", "seq"), "tp"),
            P(("groups", "seq"), None),
            P("groups"),
            P("tp"),
            P("tp", None),
            P("tp", "seq"),
            P("seq", "tp"),
            P("tp"),
            P("tp"),
            P(),
        ),
        out_specs=(P(("groups", "seq"), "tp"), P(("groups", "seq"))),
        check_vma=False,
    )
```

```python
import functools
import math

import jax
import jax.numpy as jnp
from jax import lax
from jax.experimental import pallas as pl
from jax.experimental.pallas import tpu as pltpu
from jax.sharding import PartitionSpec as P

HD = 128
LANES = 128
SUB = 8
ROW_LIMIT = 64
VMEM_BYTES = 66 * 1000 * 1000

eps = 1e-05
masked = -1e30
MESH = pl.DeviceIdType.MESH


def remote(src, dst, send_sem, recv_sem, device):
    return pltpu.make_async_remote_copy(
        src_ref=src,
        dst_ref=dst,
        send_sem=send_sem,
        recv_sem=recv_sem,
        device_id=device,
        device_id_type=MESH,
    )


def largest(size, most):
    return max(w for w in range(LANES, most + 1, LANES) if size % w == 0)


def block_of(index, size, count):
    block = jnp.zeros_like(index)
    for step in range(1, count):
        block = block + (index >= step * size).astype(jnp.int32)
    return block


def layer_kernel(
    n,
    experts,
    width,
    sem_shapes,
    *refs,
):
    dma = pltpu.SemaphoreType.DMA
    pl.run_scoped(
        functools.partial(layer_body, n, experts, width, len(sem_shapes), *refs),
        *[dma(shape) for shape in sem_shapes],
    )


def layer_body(
    n,
    experts,
    width,
    sem_count,
    *refs,
):
    sems, refs = refs[len(refs) - sem_count :], refs[: len(refs) - sem_count]
    inputs, (out_ref, val_ref) = refs[:13], refs[13:15]
    places, scratch = refs[15:24], refs[24:]
    q_ref, stream_ref, routes_ref, len_ref = places[:4]
    gain_ref, router_ref, fgain_ref, vw_ref, bias_ref = places[4:]
    order = (1, 0, 4, 5, 6, 7, 10, 11, 12)
    wup_ref, wdn_ref = inputs[8], inputs[9]
    (
    wup_v,
    wdn_v,
    kvbuf,
    hid,
    xsend,
    xin,
    xtail_send,
    xtail,
    xall,
    uown,
    usend,
    uin,
    active,
    rsend,
    rin,
    small_send,
    small_in,
    sq_send,
    sq_in,
    ) = scratch
    (
    wup_sem,
    wdn_sem,
    kv_ss,
    kv_rs,
    x_ss,
    x_rs,
    u_ss,
    u_rs,
    r_ss,
    r_rs,
    s_ss,
    s_rs,
    t_ss,
    t_rs,
    in_sem,
    ) = sems
    group = lax.axis_index("groups")
    me = lax.axis_index("seq")
    core = lax.axis_index("tp")
    partner = (group, me, 1 - core)
    rows, half = stream_ref.shape
    cap = rows // 2
    owners = n // experts
    up_chunks, up_rows, units = wup_v.shape
    down_chunks, _, down_cols = wdn_v.shape
    parts, _, part_units = usend.shape
    kv_heads = kvbuf.shape[3] // HD
    per_group = half // HD // kv_heads
    keys = n * rows
    others = pl.ds(0, n - 1)

    def up_copy(c):
        span = pl.ds(pl.multiple_of(c * up_rows, LANES), up_rows)
        return pltpu.make_async_copy(wup_ref.at[span, :], wup_v.at[c], wup_sem.at[c])

    def down_copy(c):
        cols = pl.ds(pl.multiple_of(c * down_cols, LANES), down_cols)
        return pltpu.make_async_copy(wdn_ref.at[:, cols], wdn_v.at[c], wdn_sem.at[c])

    def other(step):
        return step + (step >= me).astype(jnp.int32)

    kvbuf[...] = jnp.zeros_like(kvbuf)
    barrier = pltpu.get_barrier_semaphore()
    for step in range(n - 1):
        pl.semaphore_signal(
            barrier, inc=1, device_id=(group, other(step), core), device_id_type=MESH
        )
    pl.semaphore_signal(barrier, inc=1, device_id=partner, device_id_type=MESH)
    fetches = [
        pltpu.make_async_copy(inputs[2 + which], kvbuf.at[me, which], in_sem.at[which])
        for which in range(2)
    ] + [
        pltpu.make_async_copy(inputs[number], place, in_sem.at[2 + spot])
        for spot, (number, place) in enumerate(zip(order, places))
    ]
    for copy in fetches:
        copy.start()
    for copy in fetches:
        copy.wait()
    for c in range(up_chunks):
        up_copy(c).start()
    pl.semaphore_wait(barrier, n)

    def kv_copy(block, step, to):
        return remote(
            kvbuf.at[block], kvbuf.at[block], kv_ss.at[step], kv_rs.at[block], (group, to, core)
        )

    for step in range(n - 1, 0, -1):

        @pl.when(me + step < n)
        def _(step=step):
            kv_copy(me, step, lax.rem(me + step, n)).start()

    later = lax.broadcasted_iota(jnp.int32, (rows, rows), 0)
    sooner = lax.broadcasted_iota(jnp.int32, (rows, rows), 1)

    def upright(line):
        spread = jnp.where(later == sooner, line.astype(jnp.float32), 0.0)
        return jnp.sum(spread, axis=1, keepdims=True).astype(jnp.int32)

    route0 = upright(routes_ref[0:1, :])
    route1 = upright(routes_ref[1:2, :])
    lower = (sooner < later).astype(jnp.float32).astype(jnp.bfloat16)

    def slots(count, per_expert):
        place = lax.broadcasted_iota(jnp.int32, (rows, count * cap), 1)
        block = block_of(place, cap, count)
        expert = block_of(block, per_expert, experts)
        slot = (place - block * cap).astype(jnp.float32)
        hits = ((route0 == expert) | (route1 == expert)).astype(jnp.float32)
        rank = jnp.dot(lower, hits.astype(jnp.bfloat16), preferred_element_type=jnp.float32)
        return expert, rank == slot

    expert, at_slot = slots(experts, 1)
    placing = (((route0 == expert) | (route1 == expert)) & at_slot).astype(jnp.float32)
    placed = placing.astype(jnp.bfloat16)
    expert_r, at_slot_r = slots(n, owners)
    fetch0 = ((route0 == expert_r) & at_slot_r).astype(jnp.float32)
    fetch1 = ((route1 == expert_r) & at_slot_r).astype(jnp.float32)
    fetch = jnp.concatenate([fetch0, fetch1], axis=0).astype(jnp.bfloat16)

    for step in range(n - 1, 0, -1):

        @pl.when(step <= me)
        def _(step=step):
            kv_copy(lax.rem(me + n - step, n), step, me).wait_recv()

    for c in range(down_chunks):
        down_copy(c).start()

    def pack(values):
        return lax.dot_general(
            placed,
            values.astype(jnp.bfloat16),
            (((0,), (0,)), ((), ())),
            preferred_element_type=jnp.float32,
        )

    def dispatch(src_of, dst, send_sem, recv_sem):
        for step in range(n - 1):
            to = other(step)
            remote(src_of(to // owners), dst, send_sem, recv_sem, (group, to, core)).start()

    inv_root = 1.0 / math.sqrt(HD)
    query_row = lax.broadcasted_iota(jnp.int32, (per_group, rows, keys), 1).reshape(
        per_group * rows, keys
    )
    key_pos = lax.broadcasted_iota(jnp.int32, (per_group * rows, keys), 1)
    allowed = (key_pos <= me * rows + query_row) & (key_pos < len_ref[0])
    all_scores = []
    for head in range(kv_heads):
        cols = slice(head * HD, (head + 1) * HD)
        k_head = kvbuf[:, 0, :, cols].astype(jnp.float32).reshape(keys, HD).astype(jnp.bfloat16)
        base = head * per_group
        q_head = jnp.concatenate(
            [
                q_ref[:, (base + g) * HD : (base + g + 1) * HD].astype(jnp.float32)
                for g in range(per_group)
            ],
            axis=0,
        ).astype(jnp.bfloat16)
        all_scores.append(
            lax.dot_general(
                q_head, k_head, (((1,), (1,)), ((), ())), preferred_element_type=jnp.float32
            )
            * inv_root
        )
    updates = []
    for head in range(kv_heads):
        cols = slice(head * HD, (head + 1) * HD)
        v_head = kvbuf[:, 1, :, cols].astype(jnp.float32).reshape(keys, HD).astype(jnp.bfloat16)
        scores = jnp.where(allowed, all_scores[head], masked)
        top = jnp.max(scores, axis=-1, keepdims=True)
        weights = jnp.where(allowed, jnp.exp(scores - top), 0.0)
        total = jnp.sum(weights, axis=-1, keepdims=True)
        update = jnp.dot(weights.astype(jnp.bfloat16), v_head, preferred_element_type=jnp.float32)
        updates.append(update / total)
    squares = jnp.zeros((rows, 1), jnp.float32)
    chunks = []
    for c in range(up_chunks):
        span = slice(c * up_rows, (c + 1) * up_rows)
        update = jnp.concatenate(
            [updates[c][g * rows : (g + 1) * rows] for g in range(per_group)], axis=1
        )
        hidden = stream_ref[:, span].astype(jnp.float32) + update
        hid[:, span] = hidden
        gained = hidden * gain_ref[:, span]
        chunks.append(gained)
        squares = squares + jnp.sum(hidden * hidden, axis=1, keepdims=True)
        packed = pack(gained)
        for e in range(experts):
            xsend[c, e] = packed[e * cap : (e + 1) * cap].astype(jnp.bfloat16)
        dispatch(lambda e: xsend.at[c, e], xin.at[c, me], x_ss.at[0], x_rs.at[c])
        xin[c, me] = xsend[c, me // owners]
    lane = lax.broadcasted_iota(jnp.int32, (rows, LANES), 1)
    high = squares.astype(jnp.bfloat16).astype(jnp.float32)
    tail = jnp.where(lane == 0, high, jnp.where(lane == 1, squares - high, 0.0))
    packed = pack(tail)
    for e in range(experts):
        xtail_send[e] = packed[e * cap : (e + 1) * cap].astype(jnp.bfloat16)
    dispatch(lambda e: xtail_send.at[e], xtail.at[me], t_ss.at[0], t_rs.at[0])
    xtail[me] = xtail_send[me // owners]

    stats = jnp.where(lane == experts, squares, 0.0)
    for e in range(experts):
        part = jnp.zeros((rows, 1), jnp.float32)
        for c in range(up_chunks):
            weight = router_ref[e : e + 1, c * up_rows : (c + 1) * up_rows]
            part = part + jnp.sum(chunks[c] * weight, axis=1, keepdims=True)
        stats = jnp.where(lane == e, part, stats)
    small_send[0] = stats
    stat_copy = remote(small_send.at[0], small_in.at[0], s_ss.at[0], s_rs.at[0], partner)
    stat_copy.start()

    def arrival(block, recv_sem):
        return remote(block, block, x_ss.at[0], recv_sem, partner)

    def gather_rows(c):
        arrival(xin.at[c, others], x_rs.at[c]).wait_recv()
        arrived = jnp.concatenate([xin[c, d].astype(jnp.float32) for d in range(n)], axis=0)
        up_copy(c).wait()
        return arrived.astype(jnp.bfloat16)

    def exchange(p):
        return remote(usend.at[p], uin.at[p], u_ss.at[p], u_rs.at[p], partner)

    for c in range(up_chunks - 1):
        xall[...] = gather_rows(c)
        term = jnp.dot(xall[...], wup_v[c], preferred_element_type=jnp.float32)
        uown[...] = term if c == 0 else uown[...] + term

    xall[...] = gather_rows(up_chunks - 1)
    arrival(xtail.at[others], t_rs.at[0]).wait_recv()
    ends = jnp.concatenate([xtail[d].astype(jnp.float32) for d in range(n)], axis=0)
    sq_send[...] = jnp.broadcast_to(ends[:, 0:1] + ends[:, 1:2], sq_send.shape)
    sq_copy = remote(sq_send, sq_in, s_ss.at[1], s_rs.at[1], partner)
    sq_copy.start()
    def last_term(p):
        cols = slice(p * part_units, (p + 1) * part_units)
        return uown[:, cols] + jnp.dot(
            xall[...], wup_v[up_chunks - 1, :, cols], preferred_element_type=jnp.float32
        )

    ready = last_term(0)
    for p in range(parts):
        after = last_term(p + 1) if p + 1 < parts else None
        uown[:, p * part_units : (p + 1) * part_units] = ready
        usend[p] = ready.astype(jnp.bfloat16)
        exchange(p).start()
        ready = after

    sq_copy.wait_recv()
    scale = lax.rsqrt((sq_send[...] + sq_in[...])[:, 0:1] / width + eps)

    def activate(p):
        exchange(p).wait_recv()
        cols = slice(p * part_units, (p + 1) * part_units)
        up = (uown[:, cols] + uin[p].astype(jnp.float32)) * scale
        active[:, cols] = (up / (1.0 + jnp.exp(-up))).astype(jnp.bfloat16)

    def send_back(c, down):
        for d in range(n):
            rsend[c, d] = down[d * cap : (d + 1) * cap].astype(jnp.bfloat16)
        for step in range(n - 1):
            to = other(step)
            remote(
                rsend.at[c, to], rin.at[c, me], r_ss.at[0], r_rs.at[c], (group, to, core)
            ).start()
        rin[c, me] = rsend[c, me]

    first = min(2, down_chunks)
    downs = [None] * first
    for p in range(parts):
        activate(p)
        span = slice(p * part_units, (p + 1) * part_units)
        for c in range(first):
            if p == 0:
                down_copy(c).wait()
            term = jnp.dot(active[:, span], wdn_v[c, span], preferred_element_type=jnp.float32)
            downs[c] = term if p == 0 else downs[c] + term
    for c in range(first):
        send_back(c, downs[c])
    for c in range(first, down_chunks):
        down_copy(c).wait()
        send_back(c, jnp.dot(active[...], wdn_v[c], preferred_element_type=jnp.float32))

    stat_copy.wait_recv()
    both = small_send[0] + small_in[0]
    norm_scale = lax.rsqrt(both[:, experts : experts + 1] / width + eps)
    logits = both * norm_scale
    picked0 = jnp.sum(jnp.where(lane == route0, logits, 0.0), axis=1, keepdims=True)
    picked1 = jnp.sum(jnp.where(lane == route1, logits, 0.0), axis=1, keepdims=True)
    gate0 = 1.0 / (1.0 + jnp.exp(picked1 - picked0))
    gate1 = 1.0 / (1.0 + jnp.exp(picked0 - picked1))

    sq_part = jnp.zeros((rows, 1), jnp.float32)
    dot_part = jnp.zeros((rows, 1), jnp.float32)
    for c in range(down_chunks):
        arrival(rin.at[c, others], r_rs.at[c]).wait_recv()
        pieces = jnp.concatenate([rin[c, d].astype(jnp.float32) for d in range(n)], axis=0)
        fetched = jnp.dot(fetch, pieces.astype(jnp.bfloat16), preferred_element_type=jnp.float32)
        cols = slice(c * down_cols, (c + 1) * down_cols)
        final = hid[:, cols] + (gate0 * fetched[:rows] + gate1 * fetched[rows:])
        out_ref[:, cols] = final.astype(jnp.bfloat16)
        sq_part = sq_part + jnp.sum(final * final, axis=1, keepdims=True)
        dot_part = dot_part + jnp.sum(
            final * (fgain_ref[:, cols] * vw_ref[:, cols]), axis=1, keepdims=True
        )
    small_send[1] = jnp.where(lane == 0, sq_part, jnp.where(lane == 1, dot_part, 0.0))
    last = remote(small_send.at[1], small_in.at[1], s_ss.at[2], s_rs.at[2], partner)
    last.start()

    def sent(block, send_sem):
        remote(block, block, send_sem, r_rs.at[0], partner).wait_send()

    for step in range(1, n):

        @pl.when(me + step < n)
        def _(step=step):
            kv_copy(me, step, me).wait_send()

    sent(xin.at[:, others], x_ss.at[0])
    sent(xtail.at[others], t_ss.at[0])
    sent(rin.at[:, others], r_ss.at[0])
    for p in range(parts):
        exchange(p).wait_send()
    stat_copy.wait_send()
    sq_copy.wait_send()
    last.wait_recv()
    ends = small_send[1] + small_in[1]
    estimate = ends[:, 1:2] * lax.rsqrt(ends[:, 0:1] / width + eps) + bias_ref[0]
    place = me * rows + lax.broadcasted_iota(jnp.int32, (rows, 1), 0)
    estimate = jnp.where(place < len_ref[0], estimate, 0.0)
    val_ref[...] = jnp.sum(jnp.where(later == sooner, estimate, 0.0), axis=0, keepdims=True)
    last.wait_send()


def store_kernel(out_ref, val_ref, out_hbm, val_hbm, sem):
    copies = [
        pltpu.make_async_copy(out_ref, out_hbm, sem.at[0]),
        pltpu.make_async_copy(val_ref, val_hbm, sem.at[1]),
    ]
    for copy in copies:
        copy.start()
    for copy in copies:
        copy.wait()


def fused(
    stream,
    queries,
    key_rows,
    value_rows,
    routes,
    seq_length,
    norm_gain,
    router,
    w_up,
    w_down,
    final_gain,
    value_weight,
    value_bias,
):
    rows, half = stream.shape
    n = lax.axis_size("seq")
    experts = router.shape[1]
    hidden_units = w_up.shape[1]
    cap = rows // 2
    arrivals = n * cap
    kv_cols = key_rows.shape[1]
    up_chunks = kv_cols // HD
    up_rows = half // up_chunks
    down_cols = largest(half, 512)
    down_chunks = half // down_cols
    parts = 4
    part_units = hidden_units // parts
    vmem = pl.BlockSpec(memory_space=pltpu.VMEM)
    hbm = pl.BlockSpec(memory_space=pltpu.HBM)
    raw = pl.BlockSpec(memory_space=pl.ANY)
    bf16, f32 = jnp.bfloat16, jnp.float32
    dma = pltpu.SemaphoreType.DMA
    sem_shapes = (
        (up_chunks,),
        (down_chunks,),
        (n,),
        (n,),
        (1,),
        (up_chunks,),
        (parts,),
        (parts,),
        (1,),
        (down_chunks,),
        (3,),
        (3,),
        (1,),
        (1,),
        (11,),
    )
    out, values = pl.pallas_call(
        functools.partial(
            layer_kernel, n, experts, half * lax.axis_size("tp"), sem_shapes
        ),
        out_shape=(pltpu.VMEM((rows, half), bf16), pltpu.VMEM((1, rows), f32)),
        in_specs=[hbm] * 13,
        out_specs=(vmem, vmem),
        scratch_shapes=[
            pltpu.VMEM(stream.shape, bf16),
            pltpu.VMEM(stream.shape, bf16),
            pltpu.VMEM((2, rows), jnp.int32),
            pltpu.SMEM((1,), jnp.int32),
            pltpu.VMEM((1, half), f32),
            pltpu.VMEM((experts, half), f32),
            pltpu.VMEM((1, half), f32),
            pltpu.VMEM((1, half), f32),
            pltpu.SMEM((1,), f32),
            pltpu.VMEM((up_chunks, up_rows, hidden_units), bf16),
            pltpu.VMEM((down_chunks, hidden_units, down_cols), bf16),
            pltpu.VMEM((n, 2, rows, kv_cols), bf16),
            pltpu.VMEM((rows, half), f32),
            pltpu.VMEM((up_chunks, experts, cap, up_rows), bf16),
            pltpu.VMEM((up_chunks, n, cap, up_rows), bf16),
            pltpu.VMEM((experts, cap, LANES), bf16),
            pltpu.VMEM((n, cap, LANES), bf16),
            pltpu.VMEM((arrivals, up_rows), bf16),
            pltpu.VMEM((arrivals, hidden_units), f32),
            pltpu.VMEM((parts, arrivals, part_units), bf16),
            pltpu.VMEM((parts, arrivals, part_units), bf16),
            pltpu.VMEM((arrivals, hidden_units), bf16),
            pltpu.VMEM((down_chunks, n, cap, down_cols), bf16),
            pltpu.VMEM((down_chunks, n, cap, down_cols), bf16),
            pltpu.VMEM((2, rows, LANES), f32),
            pltpu.VMEM((2, rows, LANES), f32),
            pltpu.VMEM((arrivals, LANES), f32),
            pltpu.VMEM((arrivals, LANES), f32),
        ],
        compiler_params=pltpu.CompilerParams(
            collective_id=0, has_side_effects=True, vmem_limit_bytes=VMEM_BYTES
        ),
        name="layer",
    )(
        stream,
        queries,
        key_rows,
        value_rows,
        routes.T,
        seq_length,
        norm_gain.reshape(1, half),
        router.T,
        w_up,
        w_down,
        final_gain.reshape(1, half),
        value_weight.reshape(1, half),
        value_bias,
    )
    out, values = pl.pallas_call(
        store_kernel,
        out_shape=(
            jax.ShapeDtypeStruct((rows, half), bf16),
            jax.ShapeDtypeStruct((1, rows), f32),
        ),
        in_specs=[raw, raw],
        out_specs=(hbm, hbm),
        scratch_shapes=[dma((2,))],
        name="store",
    )(
        pltpu.with_memory_space_constraint(out, pltpu.VMEM),
        pltpu.with_memory_space_constraint(values, pltpu.VMEM),
    )
    return out, values.reshape(rows)


def unfused(
    stream,
    queries,
    key_rows,
    value_rows,
    routes,
    seq_length,
    norm_gain,
    router,
    w_up,
    w_down,
    final_gain,
    value_weight,
    value_bias,
):
    row_count = stream.shape[0]
    half_width = stream.shape[1]
    width = half_width * lax.axis_size("tp")
    experts = router.shape[1]
    seq_devices = lax.axis_size("seq")
    owners = seq_devices // experts
    my_index = lax.axis_index("seq")
    seq_limit = seq_length[0]
    positions = my_index * row_count + jnp.arange(row_count, dtype=jnp.int32)
    kv_heads = key_rows.shape[1] // HD
    per_group = queries.shape[1] // HD // kv_heads
    grouped = queries.reshape(row_count, kv_heads, per_group, HD)
    inv_root = 1.0 / math.sqrt(HD)
    slot_cap = row_count // 2
    run_max = jnp.full((kv_heads, per_group, row_count), masked, jnp.float32)
    key_block = lax.all_gather(key_rows, "seq", axis=0, tiled=True)
    value_block = lax.all_gather(value_rows, "seq", axis=0, tiled=True)
    key_count = key_block.shape[0]
    scores = (
        jnp.einsum(
            "qkgd,ckd->kgqc",
            grouped,
            key_block.reshape(key_count, kv_heads, HD),
            preferred_element_type=jnp.float32,
        )
        * inv_root
    )
    key_pos = jnp.arange(key_count, dtype=jnp.int32)
    allowed = (key_pos[None, :] <= positions[:, None]) & (key_pos[None, :] < seq_limit)
    scores = jnp.where(allowed, scores, masked)
    new_max = jnp.maximum(run_max, jnp.max(scores, axis=-1))
    weights = jnp.where(allowed, jnp.exp(scores - new_max[..., None]), 0.0)
    new_sum = jnp.sum(weights, axis=-1)
    update = jnp.einsum(
        "kgqc,ckd->kgqd",
        weights.astype(jnp.bfloat16),
        value_block.reshape(key_count, kv_heads, HD),
        preferred_element_type=jnp.float32,
    )
    attended = (update / new_sum[..., None]).transpose(2, 0, 1, 3).reshape(row_count, half_width)
    hidden = stream.astype(jnp.float32) + attended
    gained = hidden * norm_gain
    squares = jnp.sum(hidden * hidden, axis=1)
    total_sq = lax.psum(squares, "tp")
    norm_scale = lax.rsqrt(total_sq / width + eps)
    normed = gained * norm_scale[:, None]
    logits = lax.psum(jnp.dot(normed, router, precision=lax.Precision.HIGHEST), "tp")
    normed_half = normed.astype(jnp.bfloat16)
    expert_ids = jnp.arange(experts, dtype=jnp.int32)
    chosen = (routes[:, :, None] == expert_ids).astype(jnp.float32)
    picked = jnp.sum(chosen * logits[:, None, :], axis=2)
    gates = jax.nn.sigmoid(picked - picked[:, ::-1])
    flat_hits = chosen.reshape(row_count * 2, experts)
    earlier = jnp.cumsum(flat_hits, axis=0) - flat_hits
    slot_index = jnp.sum(earlier * flat_hits, axis=1).astype(jnp.int32)
    target = routes.reshape(row_count * 2) * slot_cap + slot_index
    placing = (target[:, None] == jnp.arange(experts * slot_cap, dtype=jnp.int32)[None, :]).astype(
        jnp.bfloat16
    )
    doubled = jnp.repeat(normed_half, 2, axis=0)
    packed = jnp.einsum("pe,pd->ed", placing, doubled, preferred_element_type=jnp.float32).astype(
        jnp.bfloat16
    )
    outgoing = jnp.broadcast_to(
        packed.reshape(experts, 1, slot_cap, half_width), (experts, owners, slot_cap, half_width)
    ).reshape(seq_devices, slot_cap, half_width)
    arrived = lax.all_to_all(outgoing, "seq", split_axis=0, concat_axis=0, tiled=True)
    lead = arrived.shape[0]
    items = arrived.shape[1]
    flat_rows = arrived.reshape(lead * items, half_width)
    up_part = jnp.dot(flat_rows, w_up, preferred_element_type=jnp.float32)
    up_total = lax.psum(up_part.astype(jnp.bfloat16), "tp").astype(jnp.float32)
    active = jax.nn.silu(up_total).astype(jnp.bfloat16)
    down_part = jnp.dot(active, w_down, preferred_element_type=jnp.float32).astype(jnp.bfloat16)
    partial_out = down_part.reshape(lead, items, half_width)
    returned = lax.all_to_all(partial_out, "seq", split_axis=0, concat_axis=0, tiled=True)
    summed = jnp.sum(
        returned.reshape(experts, owners, slot_cap, half_width), axis=1, dtype=jnp.float32
    ).reshape(experts * slot_cap, half_width)
    fetched = jnp.dot(placing.astype(jnp.float32), summed, precision=lax.Precision.HIGHEST)
    mixed = jnp.sum(fetched.reshape(row_count, 2, half_width) * gates[:, :, None], axis=1)
    final = hidden + mixed
    sq_part = jnp.sum(final * final, axis=1)
    dot_part = jnp.sum(final * (final_gain * value_weight), axis=1)
    sq_total, dot_total = lax.psum((sq_part, dot_part), "tp")
    estimate = dot_total * lax.rsqrt(sq_total / width + eps) + value_bias[0]
    estimate = jnp.where(positions < seq_limit, estimate, 0.0)
    return (final.astype(jnp.bfloat16), estimate)


def on_device(*args):
    stream, w_up = args[0], args[8]
    arrivals = lax.axis_size("seq") * (stream.shape[0] // 2)
    weight_bytes = 4 * w_up.shape[0] * w_up.shape[1]
    small = arrivals <= ROW_LIMIT and weight_bytes <= 52 * 1024 * 1024
    return fused(*args) if small else unfused(*args)


def solution(mesh):
    return jax.shard_map(
        on_device,
        mesh=mesh,
        in_specs=(
            P(("groups", "seq"), "tp"),
            P(("groups", "seq"), "tp"),
            P(("groups", "seq"), "tp"),
            P(("groups", "seq"), "tp"),
            P(("groups", "seq"), None),
            P("groups"),
            P("tp"),
            P("tp", None),
            P("tp", "seq"),
            P("seq", "tp"),
            P("tp"),
            P("tp"),
            P(),
        ),
        out_specs=(P(("groups", "seq"), "tp"), P(("groups", "seq"))),
        check_vma=False,
    )
```

```python
import functools
import math

import jax
import jax.numpy as jnp
from jax import lax
from jax.experimental import pallas as pl
from jax.experimental.pallas import tpu as pltpu
from jax.sharding import PartitionSpec as P

HD = 128
LANES = 128
TILE = 256
ACCS = 16
ROW_LIMIT = 64
VMEM_BYTES = 66 * 1000 * 1000

eps = 1e-05
masked = -1e30
MESH = pl.DeviceIdType.MESH


def remote(src, dst, send_sem, recv_sem, device):
    return pltpu.make_async_remote_copy(
        src_ref=src,
        dst_ref=dst,
        send_sem=send_sem,
        recv_sem=recv_sem,
        device_id=device,
        device_id_type=MESH,
    )


def largest(size, most):
    return max(w for w in range(LANES, most + 1, LANES) if size % w == 0)


def block_of(index, size, count):
    block = jnp.zeros_like(index)
    for step in range(1, count):
        block = block + (index >= step * size).astype(jnp.int32)
    return block


def layer_kernel(
    n,
    experts,
    width,
    arrivals,
    att_rows,
    sem_shapes,
    *refs,
):
    dma = pltpu.SemaphoreType.DMA
    accumulators = [pltpu.ACC(spot % 2)((arrivals, TILE), jnp.float32) for spot in range(ACCS)]
    accumulators += [pltpu.ACC(unit)((att_rows, TILE), jnp.float32) for unit in range(2)]
    pl.run_scoped(
        functools.partial(layer_body, n, experts, width, len(sem_shapes), *refs),
        *[dma(shape) for shape in sem_shapes],
        *accumulators,
    )


def layer_body(
    n,
    experts,
    width,
    sem_count,
    *refs,
):
    accs, att_accs = refs[len(refs) - ACCS - 2 : len(refs) - 2], refs[len(refs) - 2 :]
    refs = refs[: len(refs) - ACCS - 2]
    sems, refs = refs[len(refs) - sem_count :], refs[: len(refs) - sem_count]
    inputs, (out_ref, val_ref) = refs[:13], refs[13:15]
    places, scratch = refs[15:24], refs[24:]
    q_ref, stream_ref, routes_ref, len_ref = places[:4]
    gain_ref, router_ref, fgain_ref, vw_ref, bias_ref = places[4:]
    order = (1, 0, 4, 5, 6, 7, 10, 11, 12)
    wup_ref, wdn_ref = inputs[8], inputs[9]
    (
    wup_v,
    wdn_v,
    kvbuf,
    hid,
    xsend,
    xin,
    xtail_send,
    xtail,
    xall,
    uown,
    usend,
    uin,
    active,
    rsend,
    rin,
    small_send,
    small_in,
    sq_send,
    sq_in,
    ktile,
    vtile,
    ) = scratch
    (
    wup_sem,
    wdn_sem,
    kv_ss,
    kv_rs,
    x_ss,
    x_rs,
    u_ss,
    u_rs,
    r_ss,
    r_rs,
    s_ss,
    s_rs,
    t_ss,
    t_rs,
    in_sem,
    ) = sems
    group = lax.axis_index("groups")
    me = lax.axis_index("seq")
    core = lax.axis_index("tp")
    partner = (group, me, 1 - core)
    rows, half = stream_ref.shape
    cap = rows // 2
    owners = n // experts
    up_chunks, up_rows, units = wup_v.shape
    down_chunks, _, down_cols = wdn_v.shape
    parts, _, part_units = usend.shape
    kv_heads = kvbuf.shape[3] // HD
    per_group = half // HD // kv_heads
    keys = n * rows
    others = pl.ds(0, n - 1)

    def up_copy(c):
        span = pl.ds(pl.multiple_of(c * up_rows, LANES), up_rows)
        return pltpu.make_async_copy(wup_ref.at[span, :], wup_v.at[c], wup_sem.at[c])

    def down_copy(c):
        cols = pl.ds(pl.multiple_of(c * down_cols, LANES), down_cols)
        return pltpu.make_async_copy(wdn_ref.at[:, cols], wdn_v.at[c], wdn_sem.at[c])

    def other(step):
        return step + (step >= me).astype(jnp.int32)

    turn = [0, 0]

    def multiply(acc, unit, lhs, rhs, transpose=False):
        register = turn[unit] % 2
        turn[unit] += 1
        pltpu.matmul_push_rhs(
            rhs, staging_register=register, mxu_index=unit, transpose=transpose
        )
        pltpu.matmul_acc_lhs(acc, lhs, load_staged_rhs=register)

    def accumulate(spot, lhs, rhs):
        multiply(accs[spot], spot % 2, lhs, rhs)

    kvbuf[...] = jnp.zeros_like(kvbuf)
    ktile[...] = jnp.zeros_like(ktile)
    vtile[...] = jnp.zeros_like(vtile)
    barrier = pltpu.get_barrier_semaphore()
    for acc in (*accs, *att_accs):
        pltpu.matmul_pop(acc)
    for step in range(n - 1):
        pl.semaphore_signal(
            barrier, inc=1, device_id=(group, other(step), core), device_id_type=MESH
        )
    pl.semaphore_signal(barrier, inc=1, device_id=partner, device_id_type=MESH)
    fetches = [
        pltpu.make_async_copy(inputs[2 + which], kvbuf.at[me, which], in_sem.at[which])
        for which in range(2)
    ] + [
        pltpu.make_async_copy(inputs[number], place, in_sem.at[2 + spot])
        for spot, (number, place) in enumerate(zip(order, places))
    ]
    for copy in fetches:
        copy.start()
    for copy in fetches:
        copy.wait()
    for c in range(up_chunks):
        up_copy(c).start()
    pl.semaphore_wait(barrier, n)

    def kv_copy(block, step, to):
        return remote(
            kvbuf.at[block], kvbuf.at[block], kv_ss.at[step], kv_rs.at[block], (group, to, core)
        )

    for step in range(n - 1, 0, -1):

        @pl.when(me + step < n)
        def _(step=step):
            kv_copy(me, step, lax.rem(me + step, n)).start()

    later = lax.broadcasted_iota(jnp.int32, (rows, rows), 0)
    sooner = lax.broadcasted_iota(jnp.int32, (rows, rows), 1)

    def upright(line):
        spread = jnp.where(later == sooner, line.astype(jnp.float32), 0.0)
        return jnp.sum(spread, axis=1, keepdims=True).astype(jnp.int32)

    route0 = upright(routes_ref[0:1, :])
    route1 = upright(routes_ref[1:2, :])
    def slots(place, per_expert, count, line0, line1, axis):
        block = block_of(place, cap, count)
        expert = block_of(block, per_expert, experts)
        slot = (place - block * cap).astype(jnp.float32)
        first, second = line0 == expert, line1 == expert
        hits = (first | second).astype(jnp.float32)
        token = lax.broadcasted_iota(jnp.int32, place.shape, axis)
        rank = jnp.zeros(place.shape, jnp.float32)
        for t in range(rows - 1):
            own = hits[t : t + 1, :] if axis == 0 else hits[:, t : t + 1]
            rank = rank + jnp.where(token > t, own, 0.0)
        return first & (rank == slot), second & (rank == slot)

    upper = lax.broadcasted_iota(jnp.int32, (experts * cap, rows), 0)
    fill0, fill1 = slots(upper, 1, experts, routes_ref[0:1, :], routes_ref[1:2, :], 1)
    filled = (fill0 | fill1).astype(jnp.float32)
    across = lax.broadcasted_iota(jnp.int32, (rows, n * cap), 1)
    back0, back1 = slots(across, owners, n, route0, route1, 0)

    for step in range(n - 1, 0, -1):

        @pl.when(step <= me)
        def _(step=step):
            kv_copy(lax.rem(me + n - step, n), step, me).wait_recv()

    for c in range(down_chunks):
        down_copy(c).start()

    def pack(values):
        packed = jnp.zeros((experts * cap, values.shape[1]), jnp.float32)
        for t in range(rows):
            packed = packed + filled[:, t : t + 1] * values[t : t + 1, :]
        return packed

    def dispatch(src_of, dst, send_sem, recv_sem):
        for step in range(n - 1):
            to = other(step)
            remote(src_of(to // owners), dst, send_sem, recv_sem, (group, to, core)).start()

    inv_root = 1.0 / math.sqrt(HD)
    att_rows = per_group * rows
    query_row = lax.broadcasted_iota(jnp.int32, (per_group, rows, 2 * keys), 1).reshape(
        att_rows, 2 * keys
    )
    spread = lax.broadcasted_iota(jnp.int32, (att_rows, 2 * keys), 1)
    left = spread < keys
    key_pos = jnp.where(left, spread, spread - keys)
    allowed = (key_pos <= me * rows + query_row) & (key_pos < len_ref[0])
    pairs = kv_heads // 2

    def block(which, head):
        cols = slice(head * HD, (head + 1) * HD)
        return kvbuf[:, which, :, cols].astype(jnp.float32).reshape(keys, HD).astype(jnp.bfloat16)

    for pair in range(pairs):
        for side in range(2):
            down_rows = slice(side * keys, (side + 1) * keys)
            cols = slice(side * HD, (side + 1) * HD)
            ktile[pair, down_rows, cols] = block(0, 2 * pair + side)
            vtile[pair, down_rows, cols] = block(1, 2 * pair + side)
    all_scores = []
    for pair in range(pairs):
        sides = []
        for side in range(2):
            base = (2 * pair + side) * per_group
            sides.append(
                jnp.concatenate(
                    [
                        q_ref[:, (base + g) * HD : (base + g + 1) * HD].astype(jnp.float32)
                        for g in range(per_group)
                    ],
                    axis=0,
                ).astype(jnp.bfloat16)
            )
        unit = pair % 2
        multiply(
            att_accs[unit], unit, jnp.concatenate(sides, axis=1), ktile[pair], transpose=True
        )
        if unit or pair == pairs - 1:
            for done in range(pair - unit, pair + 1):
                all_scores.append(pltpu.matmul_pop(att_accs[done % 2])[:, : 2 * keys] * inv_root)
    all_weights, totals = [], []
    for pair in range(pairs):
        scores = jnp.where(allowed, all_scores[pair], masked)
        tops = [
            jnp.max(jnp.where(mine, scores, masked), axis=-1, keepdims=True)
            for mine in (left, ~left)
        ]
        weights = jnp.where(allowed, jnp.exp(scores - jnp.where(left, tops[0], tops[1])), 0.0)
        totals += [
            jnp.sum(jnp.where(mine, weights, 0.0), axis=-1, keepdims=True)
            for mine in (left, ~left)
        ]
        wide = [weights]
        if 2 * keys < TILE:
            wide.append(jnp.zeros((att_rows, TILE - 2 * keys), jnp.float32))
        all_weights.append(jnp.concatenate(wide, axis=1).astype(jnp.bfloat16))
    updates = []
    for pair in range(pairs):
        unit = pair % 2
        multiply(att_accs[unit], unit, all_weights[pair], vtile[pair])
        if unit or pair == pairs - 1:
            for done in range(pair - unit, pair + 1):
                both_sides = pltpu.matmul_pop(att_accs[done % 2])
                for side in range(2):
                    update = both_sides[:, side * HD : (side + 1) * HD]
                    updates.append(update / totals[2 * done + side])
    squares = jnp.zeros((rows, 1), jnp.float32)
    chunks = []
    for c in range(up_chunks):
        span = slice(c * up_rows, (c + 1) * up_rows)
        update = jnp.concatenate(
            [updates[c][g * rows : (g + 1) * rows] for g in range(per_group)], axis=1
        )
        hidden = stream_ref[:, span].astype(jnp.float32) + update
        hid[:, span] = hidden
        gained = hidden * gain_ref[:, span]
        chunks.append(gained)
        squares = squares + jnp.sum(hidden * hidden, axis=1, keepdims=True)
        packed = pack(gained)
        for e in range(experts):
            xsend[c, e] = packed[e * cap : (e + 1) * cap].astype(jnp.bfloat16)
        dispatch(lambda e: xsend.at[c, e], xin.at[c, me], x_ss.at[0], x_rs.at[c])
        xin[c, me] = xsend[c, me // owners]
    lane = lax.broadcasted_iota(jnp.int32, (rows, LANES), 1)
    high = squares.astype(jnp.bfloat16).astype(jnp.float32)
    tail = jnp.where(lane == 0, high, jnp.where(lane == 1, squares - high, 0.0))
    packed = pack(tail)
    for e in range(experts):
        xtail_send[e] = packed[e * cap : (e + 1) * cap].astype(jnp.bfloat16)
    dispatch(lambda e: xtail_send.at[e], xtail.at[me], t_ss.at[0], t_rs.at[0])
    xtail[me] = xtail_send[me // owners]

    stats = jnp.where(lane == experts, squares, 0.0)
    for e in range(experts):
        part = jnp.zeros((rows, 1), jnp.float32)
        for c in range(up_chunks):
            weight = router_ref[e : e + 1, c * up_rows : (c + 1) * up_rows]
            part = part + jnp.sum(chunks[c] * weight, axis=1, keepdims=True)
        stats = jnp.where(lane == e, part, stats)
    small_send[0] = stats
    stat_copy = remote(small_send.at[0], small_in.at[0], s_ss.at[0], s_rs.at[0], partner)
    stat_copy.start()

    def arrival(block, recv_sem):
        return remote(block, block, x_ss.at[0], recv_sem, partner)

    def gather_rows(c):
        arrival(xin.at[c, others], x_rs.at[c]).wait_recv()
        arrived = jnp.concatenate([xin[c, d].astype(jnp.float32) for d in range(n)], axis=0)
        up_copy(c).wait()
        return arrived.astype(jnp.bfloat16)

    def exchange(p):
        return remote(usend.at[p], uin.at[p], u_ss.at[p], u_rs.at[p], partner)

    def up_tiles(c, spots):
        for pair in range(spots.start, spots.stop, 2):
            for k in range(up_rows // TILE):
                deep = slice(k * TILE, (k + 1) * TILE)
                for spot in (pair, pair + 1):
                    cols = slice(spot * TILE, (spot + 1) * TILE)
                    accumulate(spot, xall[:, deep], wup_v[c, deep, cols])

    for c in range(up_chunks - 1):
        xall[...] = gather_rows(c)
        up_tiles(c, range(ACCS))

    xall[...] = gather_rows(up_chunks - 1)
    arrival(xtail.at[others], t_rs.at[0]).wait_recv()
    ends = jnp.concatenate([xtail[d].astype(jnp.float32) for d in range(n)], axis=0)
    sq_send[...] = jnp.broadcast_to(ends[:, 0:1] + ends[:, 1:2], sq_send.shape)
    sq_copy = remote(sq_send, sq_in, s_ss.at[1], s_rs.at[1], partner)
    sq_copy.start()
    per_part = ACCS // parts

    def finish_part(p):
        for spot in range(p * per_part, (p + 1) * per_part):
            term = pltpu.matmul_pop(accs[spot])
            uown[:, spot * TILE : (spot + 1) * TILE] = term
            at = (spot - p * per_part) * TILE
            usend[p, :, at : at + TILE] = term.astype(jnp.bfloat16)
        exchange(p).start()

    for p in range(parts):
        at = p * per_part
        up_tiles(up_chunks - 1, range(at, at + 2))
        if p:
            finish_part(p - 1)
        up_tiles(up_chunks - 1, range(at + 2, at + per_part))
    finish_part(parts - 1)

    sq_copy.wait_recv()
    scale = lax.rsqrt((sq_send[...] + sq_in[...])[:, 0:1] / width + eps)

    def activate(p):
        cols = slice(p * part_units, (p + 1) * part_units)
        up = (uown[:, cols] + uin[p].astype(jnp.float32)) * scale
        active[:, cols] = (up / (1.0 + jnp.exp(-up))).astype(jnp.bfloat16)

    pieces_of = [(c, 0, down_cols) for c in range(down_chunks - 1)]
    pieces_of += [(down_chunks - 1, lo, down_cols // 2) for lo in (0, down_cols // 2)]

    def down_tiles(t, low, high):
        c, lo, wide = pieces_of[t]
        middle = units // TILE // 2
        for k in range(low, high):
            deep = slice(k * TILE, (k + 1) * TILE)
            if wide == TILE:
                spots = ((2 * t + k // middle, 0),)
            else:
                spots = tuple((2 * t + q, q) for q in range(wide // TILE))
            for spot, q in spots:
                cols = slice(lo + q * TILE, lo + (q + 1) * TILE)
                accumulate(spot, active[:, deep], wdn_v[c, deep, cols])

    def halves_tiles(t, low, high):
        middle = units // TILE // 2
        for k in range(low, high):
            down_tiles(t, k, k + 1)
            down_tiles(t, k + middle, k + middle + 1)

    def send_back(t):
        c, lo, wide = pieces_of[t]
        cols = pl.ds(lo, wide)
        terms = [pltpu.matmul_pop(accs[2 * t + q]) for q in range(2)]
        down = terms[0] + terms[1] if wide == TILE else jnp.concatenate(terms, axis=1)
        for d in range(n):
            rsend[c, d, :, cols] = down[d * cap : (d + 1) * cap].astype(jnp.bfloat16)
        for step in range(n - 1):
            to = other(step)
            remote(
                rsend.at[c, to, :, cols],
                rin.at[c, me, :, cols],
                r_ss.at[0],
                r_rs.at[t],
                (group, to, core),
            ).start()
        rin[c, me, :, cols] = rsend[c, me, :, cols]

    for c in range(down_chunks):
        down_copy(c).wait()
    per_part = part_units // TILE
    for p in range(parts - 1):
        exchange(p).wait_recv()
    for p in range(parts):
        if p == parts - 1:
            exchange(p).wait_recv()
        activate(p)
        for t in range(2):
            down_tiles(t, p * per_part, (p + 1) * per_part)
    send_back(0)
    depth = units // TILE
    for t in range(2, len(pieces_of)):
        if pieces_of[t][2] == TILE:
            halves_tiles(t, 0, 2)
            send_back(t - 1)
            halves_tiles(t, 2, depth // 2)
        else:
            down_tiles(t, 0, 4)
            send_back(t - 1)
            down_tiles(t, 4, depth)
    send_back(len(pieces_of) - 1)

    stat_copy.wait_recv()
    both = small_send[0] + small_in[0]
    norm_scale = lax.rsqrt(both[:, experts : experts + 1] / width + eps)
    logits = both * norm_scale
    picked0 = jnp.sum(jnp.where(lane == route0, logits, 0.0), axis=1, keepdims=True)
    picked1 = jnp.sum(jnp.where(lane == route1, logits, 0.0), axis=1, keepdims=True)
    gate0 = 1.0 / (1.0 + jnp.exp(picked1 - picked0))
    gate1 = 1.0 / (1.0 + jnp.exp(picked0 - picked1))

    coeff = gate0 * back0.astype(jnp.float32) + gate1 * back1.astype(jnp.float32)
    sq_part = jnp.zeros((rows, 1), jnp.float32)
    dot_part = jnp.zeros((rows, 1), jnp.float32)
    for t, (c, lo, wide) in enumerate(pieces_of):
        span = slice(lo, lo + wide)
        arrival(rin.at[c, others, :, span], r_rs.at[t]).wait_recv()
        cols = slice(c * down_cols + lo, c * down_cols + lo + wide)
        sums = [hid[:, cols], jnp.zeros((rows, wide), jnp.float32)]
        for d in range(n):
            piece = rin[c, d, :, span].astype(jnp.float32)
            for slot in range(cap):
                spot = d * cap + slot
                sums[slot % 2] += coeff[:, spot : spot + 1] * piece[slot : slot + 1, :]
        final = sums[0] + sums[1]
        out_ref[:, cols] = final.astype(jnp.bfloat16)
        sq_part = sq_part + jnp.sum(final * final, axis=1, keepdims=True)
        dot_part = dot_part + jnp.sum(
            final * (fgain_ref[:, cols] * vw_ref[:, cols]), axis=1, keepdims=True
        )
    small_send[1] = jnp.where(lane == 0, sq_part, jnp.where(lane == 1, dot_part, 0.0))
    last = remote(small_send.at[1], small_in.at[1], s_ss.at[2], s_rs.at[2], partner)
    last.start()

    def sent(block, send_sem):
        remote(block, block, send_sem, r_rs.at[0], partner).wait_send()

    for step in range(1, n):

        @pl.when(me + step < n)
        def _(step=step):
            kv_copy(me, step, me).wait_send()

    sent(xin.at[:, others], x_ss.at[0])
    sent(xtail.at[others], t_ss.at[0])
    sent(rin.at[:, others], r_ss.at[0])
    for p in range(parts):
        exchange(p).wait_send()
    stat_copy.wait_send()
    sq_copy.wait_send()
    last.wait_recv()
    ends = small_send[1] + small_in[1]
    estimate = ends[:, 1:2] * lax.rsqrt(ends[:, 0:1] / width + eps) + bias_ref[0]
    place = me * rows + lax.broadcasted_iota(jnp.int32, (rows, 1), 0)
    estimate = jnp.where(place < len_ref[0], estimate, 0.0)
    val_ref[...] = jnp.sum(jnp.where(later == sooner, estimate, 0.0), axis=0, keepdims=True)
    last.wait_send()


def store_kernel(out_ref, val_ref, out_hbm, val_hbm, sem):
    copies = [
        pltpu.make_async_copy(out_ref, out_hbm, sem.at[0]),
        pltpu.make_async_copy(val_ref, val_hbm, sem.at[1]),
    ]
    for copy in copies:
        copy.start()
    for copy in copies:
        copy.wait()


def fused(
    stream,
    queries,
    key_rows,
    value_rows,
    routes,
    seq_length,
    norm_gain,
    router,
    w_up,
    w_down,
    final_gain,
    value_weight,
    value_bias,
):
    rows, half = stream.shape
    n = lax.axis_size("seq")
    experts = router.shape[1]
    hidden_units = w_up.shape[1]
    cap = rows // 2
    arrivals = n * cap
    kv_cols = key_rows.shape[1]
    up_chunks = kv_cols // HD
    up_rows = half // up_chunks
    down_cols = largest(half, 512)
    down_chunks = half // down_cols
    parts = 4
    att_rows = up_rows // HD * rows
    part_units = hidden_units // parts
    vmem = pl.BlockSpec(memory_space=pltpu.VMEM)
    hbm = pl.BlockSpec(memory_space=pltpu.HBM)
    raw = pl.BlockSpec(memory_space=pl.ANY)
    bf16, f32 = jnp.bfloat16, jnp.float32
    dma = pltpu.SemaphoreType.DMA
    sem_shapes = (
        (up_chunks,),
        (down_chunks,),
        (n,),
        (n,),
        (1,),
        (up_chunks,),
        (parts,),
        (parts,),
        (1,),
        (down_chunks + 1,),
        (3,),
        (3,),
        (1,),
        (1,),
        (11,),
    )
    out, values = pl.pallas_call(
        functools.partial(
            layer_kernel, n, experts, half * lax.axis_size("tp"), arrivals, att_rows, sem_shapes
        ),
        out_shape=(pltpu.VMEM((rows, half), bf16), pltpu.VMEM((1, rows), f32)),
        in_specs=[hbm] * 13,
        out_specs=(vmem, vmem),
        scratch_shapes=[
            pltpu.VMEM(stream.shape, bf16),
            pltpu.VMEM(stream.shape, bf16),
            pltpu.VMEM((2, rows), jnp.int32),
            pltpu.SMEM((1,), jnp.int32),
            pltpu.VMEM((1, half), f32),
            pltpu.VMEM((experts, half), f32),
            pltpu.VMEM((1, half), f32),
            pltpu.VMEM((1, half), f32),
            pltpu.SMEM((1,), f32),
            pltpu.VMEM((up_chunks, up_rows, hidden_units), bf16),
            pltpu.VMEM((down_chunks, hidden_units, down_cols), bf16),
            pltpu.VMEM((n, 2, rows, kv_cols), bf16),
            pltpu.VMEM((rows, half), f32),
            pltpu.VMEM((up_chunks, experts, cap, up_rows), bf16),
            pltpu.VMEM((up_chunks, n, cap, up_rows), bf16),
            pltpu.VMEM((experts, cap, LANES), bf16),
            pltpu.VMEM((n, cap, LANES), bf16),
            pltpu.VMEM((arrivals, up_rows), bf16),
            pltpu.VMEM((arrivals, hidden_units), f32),
            pltpu.VMEM((parts, arrivals, part_units), bf16),
            pltpu.VMEM((parts, arrivals, part_units), bf16),
            pltpu.VMEM((arrivals, hidden_units), bf16),
            pltpu.VMEM((down_chunks, n, cap, down_cols), bf16),
            pltpu.VMEM((down_chunks, n, cap, down_cols), bf16),
            pltpu.VMEM((2, rows, LANES), f32),
            pltpu.VMEM((2, rows, LANES), f32),
            pltpu.VMEM((arrivals, LANES), f32),
            pltpu.VMEM((arrivals, LANES), f32),
            pltpu.VMEM((up_chunks // 2, TILE, TILE), bf16),
            pltpu.VMEM((up_chunks // 2, TILE, TILE), bf16),
        ],
        compiler_params=pltpu.CompilerParams(
            collective_id=0, has_side_effects=True, vmem_limit_bytes=VMEM_BYTES
        ),
        name="layer",
    )(
        stream,
        queries,
        key_rows,
        value_rows,
        routes.T,
        seq_length,
        norm_gain.reshape(1, half),
        router.T,
        w_up,
        w_down,
        final_gain.reshape(1, half),
        value_weight.reshape(1, half),
        value_bias,
    )
    out, values = pl.pallas_call(
        store_kernel,
        out_shape=(
            jax.ShapeDtypeStruct((rows, half), bf16),
            jax.ShapeDtypeStruct((1, rows), f32),
        ),
        in_specs=[raw, raw],
        out_specs=(hbm, hbm),
        scratch_shapes=[dma((2,))],
        name="store",
    )(
        pltpu.with_memory_space_constraint(out, pltpu.VMEM),
        pltpu.with_memory_space_constraint(values, pltpu.VMEM),
    )
    return out, values.reshape(rows)


def unfused(
    stream,
    queries,
    key_rows,
    value_rows,
    routes,
    seq_length,
    norm_gain,
    router,
    w_up,
    w_down,
    final_gain,
    value_weight,
    value_bias,
):
    row_count = stream.shape[0]
    half_width = stream.shape[1]
    width = half_width * lax.axis_size("tp")
    experts = router.shape[1]
    seq_devices = lax.axis_size("seq")
    owners = seq_devices // experts
    my_index = lax.axis_index("seq")
    seq_limit = seq_length[0]
    positions = my_index * row_count + jnp.arange(row_count, dtype=jnp.int32)
    kv_heads = key_rows.shape[1] // HD
    per_group = queries.shape[1] // HD // kv_heads
    grouped = queries.reshape(row_count, kv_heads, per_group, HD)
    inv_root = 1.0 / math.sqrt(HD)
    slot_cap = row_count // 2
    run_max = jnp.full((kv_heads, per_group, row_count), masked, jnp.float32)
    key_block = lax.all_gather(key_rows, "seq", axis=0, tiled=True)
    value_block = lax.all_gather(value_rows, "seq", axis=0, tiled=True)
    key_count = key_block.shape[0]
    scores = (
        jnp.einsum(
            "qkgd,ckd->kgqc",
            grouped,
            key_block.reshape(key_count, kv_heads, HD),
            preferred_element_type=jnp.float32,
        )
        * inv_root
    )
    key_pos = jnp.arange(key_count, dtype=jnp.int32)
    allowed = (key_pos[None, :] <= positions[:, None]) & (key_pos[None, :] < seq_limit)
    scores = jnp.where(allowed, scores, masked)
    new_max = jnp.maximum(run_max, jnp.max(scores, axis=-1))
    weights = jnp.where(allowed, jnp.exp(scores - new_max[..., None]), 0.0)
    new_sum = jnp.sum(weights, axis=-1)
    update = jnp.einsum(
        "kgqc,ckd->kgqd",
        weights.astype(jnp.bfloat16),
        value_block.reshape(key_count, kv_heads, HD),
        preferred_element_type=jnp.float32,
    )
    attended = (update / new_sum[..., None]).transpose(2, 0, 1, 3).reshape(row_count, half_width)
    hidden = stream.astype(jnp.float32) + attended
    gained = hidden * norm_gain
    squares = jnp.sum(hidden * hidden, axis=1)
    total_sq = lax.psum(squares, "tp")
    norm_scale = lax.rsqrt(total_sq / width + eps)
    normed = gained * norm_scale[:, None]
    logits = lax.psum(jnp.dot(normed, router, precision=lax.Precision.HIGHEST), "tp")
    normed_half = normed.astype(jnp.bfloat16)
    expert_ids = jnp.arange(experts, dtype=jnp.int32)
    chosen = (routes[:, :, None] == expert_ids).astype(jnp.float32)
    picked = jnp.sum(chosen * logits[:, None, :], axis=2)
    gates = jax.nn.sigmoid(picked - picked[:, ::-1])
    flat_hits = chosen.reshape(row_count * 2, experts)
    earlier = jnp.cumsum(flat_hits, axis=0) - flat_hits
    slot_index = jnp.sum(earlier * flat_hits, axis=1).astype(jnp.int32)
    target = routes.reshape(row_count * 2) * slot_cap + slot_index
    placing = (target[:, None] == jnp.arange(experts * slot_cap, dtype=jnp.int32)[None, :]).astype(
        jnp.bfloat16
    )
    doubled = jnp.repeat(normed_half, 2, axis=0)
    packed = jnp.einsum("pe,pd->ed", placing, doubled, preferred_element_type=jnp.float32).astype(
        jnp.bfloat16
    )
    outgoing = jnp.broadcast_to(
        packed.reshape(experts, 1, slot_cap, half_width), (experts, owners, slot_cap, half_width)
    ).reshape(seq_devices, slot_cap, half_width)
    arrived = lax.all_to_all(outgoing, "seq", split_axis=0, concat_axis=0, tiled=True)
    lead = arrived.shape[0]
    items = arrived.shape[1]
    flat_rows = arrived.reshape(lead * items, half_width)
    up_part = jnp.dot(flat_rows, w_up, preferred_element_type=jnp.float32)
    up_total = lax.psum(up_part.astype(jnp.bfloat16), "tp").astype(jnp.float32)
    active = jax.nn.silu(up_total).astype(jnp.bfloat16)
    down_part = jnp.dot(active, w_down, preferred_element_type=jnp.float32).astype(jnp.bfloat16)
    partial_out = down_part.reshape(lead, items, half_width)
    returned = lax.all_to_all(partial_out, "seq", split_axis=0, concat_axis=0, tiled=True)
    summed = jnp.sum(
        returned.reshape(experts, owners, slot_cap, half_width), axis=1, dtype=jnp.float32
    ).reshape(experts * slot_cap, half_width)
    fetched = jnp.dot(placing.astype(jnp.float32), summed, precision=lax.Precision.HIGHEST)
    mixed = jnp.sum(fetched.reshape(row_count, 2, half_width) * gates[:, :, None], axis=1)
    final = hidden + mixed
    sq_part = jnp.sum(final * final, axis=1)
    dot_part = jnp.sum(final * (final_gain * value_weight), axis=1)
    sq_total, dot_total = lax.psum((sq_part, dot_part), "tp")
    estimate = dot_total * lax.rsqrt(sq_total / width + eps) + value_bias[0]
    estimate = jnp.where(positions < seq_limit, estimate, 0.0)
    return (final.astype(jnp.bfloat16), estimate)


def on_device(*args):
    stream, w_up = args[0], args[8]
    arrivals = lax.axis_size("seq") * (stream.shape[0] // 2)
    weight_bytes = 4 * w_up.shape[0] * w_up.shape[1]
    kv_heads = args[2].shape[1] // HD
    keys = lax.axis_size("seq") * stream.shape[0]
    tiled = (
        w_up.shape[1] == ACCS * TILE
        and stream.shape[1] % (kv_heads * TILE) == 0
        and kv_heads % 2 == 0
        and 2 * keys <= TILE
    )
    small = tiled and arrivals <= ROW_LIMIT and weight_bytes <= 52 * 1024 * 1024
    return fused(*args) if small else unfused(*args)


def solution(mesh):
    return jax.shard_map(
        on_device,
        mesh=mesh,
        in_specs=(
            P(("groups", "seq"), "tp"),
            P(("groups", "seq"), "tp"),
            P(("groups", "seq"), "tp"),
            P(("groups", "seq"), "tp"),
            P(("groups", "seq"), None),
            P("groups"),
            P("tp"),
            P("tp", None),
            P("tp", "seq"),
            P("seq", "tp"),
            P("tp"),
            P("tp"),
            P(),
        ),
        out_specs=(P(("groups", "seq"), "tp"), P(("groups", "seq"))),
        check_vma=False,
    )
```

```python
import functools
import math

import jax
import jax.numpy as jnp
from jax import lax
from jax.experimental import pallas as pl
from jax.experimental.pallas import tpu as pltpu
from jax.sharding import PartitionSpec as P

HD = 128
LANES = 128
SUB = 8
ROW_LIMIT = 64
VMEM_BYTES = 66 * 1000 * 1000

eps = 1e-05
masked = -1e30
MESH = pl.DeviceIdType.MESH


def remote(src, dst, send_sem, recv_sem, device):
    return pltpu.make_async_remote_copy(
        src_ref=src,
        dst_ref=dst,
        send_sem=send_sem,
        recv_sem=recv_sem,
        device_id=device,
        device_id_type=MESH,
    )


def largest(size, most):
    return max(w for w in range(LANES, most + 1, LANES) if size % w == 0)


def block_of(index, size, count):
    block = jnp.zeros_like(index)
    for step in range(1, count):
        block = block + (index >= step * size).astype(jnp.int32)
    return block


def layer_kernel(
    n,
    experts,
    width,
    sem_shapes,
    *refs,
):
    dma = pltpu.SemaphoreType.DMA
    pl.run_scoped(
        functools.partial(layer_body, n, experts, width, len(sem_shapes), *refs),
        *[dma(shape) for shape in sem_shapes],
    )


def layer_body(
    n,
    experts,
    width,
    sem_count,
    *refs,
):
    sems, refs = refs[len(refs) - sem_count :], refs[: len(refs) - sem_count]
    inputs, (out_ref, val_ref) = refs[:13], refs[13:15]
    places, scratch = refs[15:24], refs[24:]
    q_ref, stream_ref, routes_ref, len_ref = places[:4]
    gain_ref, router_ref, fgain_ref, vw_ref, bias_ref = places[4:]
    order = (1, 0, 4, 5, 6, 7, 10, 11, 12)
    wup_ref, wdn_ref = inputs[8], inputs[9]
    (
    wup_v,
    wdn_v,
    kvbuf,
    hid,
    xsend,
    xin,
    xtail_send,
    xtail,
    xall,
    uown,
    usend,
    uin,
    active,
    rsend,
    rin,
    small_send,
    small_in,
    sq_send,
    sq_in,
    ) = scratch
    (
    wup_sem,
    wdn_sem,
    kv_ss,
    kv_rs,
    x_ss,
    x_rs,
    u_ss,
    u_rs,
    r_ss,
    r_rs,
    s_ss,
    s_rs,
    t_ss,
    t_rs,
    in_sem,
    ) = sems
    group = lax.axis_index("groups")
    me = lax.axis_index("seq")
    core = lax.axis_index("tp")
    partner = (group, me, 1 - core)
    rows, half = stream_ref.shape
    cap = rows // 2
    owners = n // experts
    up_chunks, up_rows, units = wup_v.shape
    down_chunks, _, down_cols = wdn_v.shape
    parts, _, part_units = usend.shape
    kv_heads = kvbuf.shape[3] // HD
    per_group = half // HD // kv_heads
    keys = n * rows
    others = pl.ds(0, n - 1)

    def up_copy(c):
        span = pl.ds(pl.multiple_of(c * up_rows, LANES), up_rows)
        return pltpu.make_async_copy(wup_ref.at[span, :], wup_v.at[c], wup_sem.at[c])

    def down_copy(c):
        cols = pl.ds(pl.multiple_of(c * down_cols, LANES), down_cols)
        return pltpu.make_async_copy(wdn_ref.at[:, cols], wdn_v.at[c], wdn_sem.at[c])

    def other(step):
        return step + (step >= me).astype(jnp.int32)

    kvbuf[...] = jnp.zeros_like(kvbuf)
    barrier = pltpu.get_barrier_semaphore()
    for step in range(n - 1):
        pl.semaphore_signal(
            barrier, inc=1, device_id=(group, other(step), core), device_id_type=MESH
        )
    pl.semaphore_signal(barrier, inc=1, device_id=partner, device_id_type=MESH)
    fetches = [
        pltpu.make_async_copy(inputs[2 + which], kvbuf.at[me, which], in_sem.at[which])
        for which in range(2)
    ] + [
        pltpu.make_async_copy(inputs[number], place, in_sem.at[2 + spot])
        for spot, (number, place) in enumerate(zip(order, places))
    ]
    for copy in fetches:
        copy.start()
    for copy in fetches:
        copy.wait()
    for c in range(up_chunks):
        up_copy(c).start()
    pl.semaphore_wait(barrier, n)

    def kv_copy(block, step, to):
        return remote(
            kvbuf.at[block], kvbuf.at[block], kv_ss.at[step], kv_rs.at[block], (group, to, core)
        )

    for step in range(n - 1, 0, -1):

        @pl.when(me + step < n)
        def _(step=step):
            kv_copy(me, step, lax.rem(me + step, n)).start()

    later = lax.broadcasted_iota(jnp.int32, (rows, rows), 0)
    sooner = lax.broadcasted_iota(jnp.int32, (rows, rows), 1)

    def upright(line):
        spread = jnp.where(later == sooner, line.astype(jnp.float32), 0.0)
        return jnp.sum(spread, axis=1, keepdims=True).astype(jnp.int32)

    route0 = upright(routes_ref[0:1, :])
    route1 = upright(routes_ref[1:2, :])
    lower = (sooner < later).astype(jnp.float32).astype(jnp.bfloat16)

    def slots(count, per_expert):
        place = lax.broadcasted_iota(jnp.int32, (rows, count * cap), 1)
        block = block_of(place, cap, count)
        expert = block_of(block, per_expert, experts)
        slot = (place - block * cap).astype(jnp.float32)
        hits = ((route0 == expert) | (route1 == expert)).astype(jnp.float32)
        rank = jnp.dot(lower, hits.astype(jnp.bfloat16), preferred_element_type=jnp.float32)
        return expert, rank == slot

    expert, at_slot = slots(experts, 1)
    placing = (((route0 == expert) | (route1 == expert)) & at_slot).astype(jnp.float32)
    placed = placing.astype(jnp.bfloat16)
    expert_r, at_slot_r = slots(n, owners)
    fetch0 = ((route0 == expert_r) & at_slot_r).astype(jnp.float32)
    fetch1 = ((route1 == expert_r) & at_slot_r).astype(jnp.float32)
    fetch = jnp.concatenate([fetch0, fetch1], axis=0).astype(jnp.bfloat16)

    for step in range(n - 1, 0, -1):

        @pl.when(step <= me)
        def _(step=step):
            kv_copy(lax.rem(me + n - step, n), step, me).wait_recv()

    for c in range(down_chunks):
        down_copy(c).start()

    def pack(values):
        return lax.dot_general(
            placed,
            values.astype(jnp.bfloat16),
            (((0,), (0,)), ((), ())),
            preferred_element_type=jnp.float32,
        )

    def dispatch(src_of, dst, send_sem, recv_sem):
        for step in range(n - 1):
            to = other(step)
            remote(src_of(to // owners), dst, send_sem, recv_sem, (group, to, core)).start()

    inv_root = 1.0 / math.sqrt(HD)
    query_row = lax.broadcasted_iota(jnp.int32, (per_group, rows, keys), 1).reshape(
        per_group * rows, keys
    )
    key_pos = lax.broadcasted_iota(jnp.int32, (per_group * rows, keys), 1)
    allowed = (key_pos <= me * rows + query_row) & (key_pos < len_ref[0])
    all_scores = []
    for head in range(kv_heads):
        cols = slice(head * HD, (head + 1) * HD)
        k_head = kvbuf[:, 0, :, cols].astype(jnp.float32).reshape(keys, HD).astype(jnp.bfloat16)
        base = head * per_group
        q_head = jnp.concatenate(
            [
                q_ref[:, (base + g) * HD : (base + g + 1) * HD].astype(jnp.float32)
                for g in range(per_group)
            ],
            axis=0,
        ).astype(jnp.bfloat16)
        all_scores.append(
            lax.dot_general(
                q_head, k_head, (((1,), (1,)), ((), ())), preferred_element_type=jnp.float32
            )
            * inv_root
        )
    updates = []
    for head in range(kv_heads):
        cols = slice(head * HD, (head + 1) * HD)
        v_head = kvbuf[:, 1, :, cols].astype(jnp.float32).reshape(keys, HD).astype(jnp.bfloat16)
        scores = jnp.where(allowed, all_scores[head], masked)
        top = jnp.max(scores, axis=-1, keepdims=True)
        weights = jnp.where(allowed, jnp.exp(scores - top), 0.0)
        total = jnp.sum(weights, axis=-1, keepdims=True)
        update = jnp.dot(weights.astype(jnp.bfloat16), v_head, preferred_element_type=jnp.float32)
        updates.append(update / total)
    squares = jnp.zeros((rows, 1), jnp.float32)
    chunks = []
    for c in range(up_chunks):
        span = slice(c * up_rows, (c + 1) * up_rows)
        update = jnp.concatenate(
            [updates[c][g * rows : (g + 1) * rows] for g in range(per_group)], axis=1
        )
        hidden = stream_ref[:, span].astype(jnp.float32) + update
        hid[:, span] = hidden
        gained = hidden * gain_ref[:, span]
        chunks.append(gained)
        squares = squares + jnp.sum(hidden * hidden, axis=1, keepdims=True)
        packed = pack(gained)
        for e in range(experts):
            xsend[c, e] = packed[e * cap : (e + 1) * cap].astype(jnp.bfloat16)
        dispatch(lambda e: xsend.at[c, e], xin.at[c, me], x_ss.at[0], x_rs.at[c])
        xin[c, me] = xsend[c, me // owners]
    lane = lax.broadcasted_iota(jnp.int32, (rows, LANES), 1)
    high = squares.astype(jnp.bfloat16).astype(jnp.float32)
    tail = jnp.where(lane == 0, high, jnp.where(lane == 1, squares - high, 0.0))
    packed = pack(tail)
    for e in range(experts):
        xtail_send[e] = packed[e * cap : (e + 1) * cap].astype(jnp.bfloat16)
    dispatch(lambda e: xtail_send.at[e], xtail.at[me], t_ss.at[0], t_rs.at[0])
    xtail[me] = xtail_send[me // owners]

    stats = jnp.where(lane == experts, squares, 0.0)
    for e in range(experts):
        part = jnp.zeros((rows, 1), jnp.float32)
        for c in range(up_chunks):
            weight = router_ref[e : e + 1, c * up_rows : (c + 1) * up_rows]
            part = part + jnp.sum(chunks[c] * weight, axis=1, keepdims=True)
        stats = jnp.where(lane == e, part, stats)
    small_send[0] = stats
    stat_copy = remote(small_send.at[0], small_in.at[0], s_ss.at[0], s_rs.at[0], partner)
    stat_copy.start()

    def arrival(block, recv_sem):
        return remote(block, block, x_ss.at[0], recv_sem, partner)

    def gather_rows(c):
        arrival(xin.at[c, others], x_rs.at[c]).wait_recv()
        arrived = jnp.concatenate([xin[c, d].astype(jnp.float32) for d in range(n)], axis=0)
        up_copy(c).wait()
        return arrived.astype(jnp.bfloat16)

    def exchange(p):
        return remote(usend.at[p], uin.at[p], u_ss.at[p], u_rs.at[p], partner)

    for c in range(up_chunks - 1):
        xall[...] = gather_rows(c)
        term = jnp.dot(xall[...], wup_v[c], preferred_element_type=jnp.float32)
        uown[...] = term if c == 0 else uown[...] + term

    xall[...] = gather_rows(up_chunks - 1)
    arrival(xtail.at[others], t_rs.at[0]).wait_recv()
    ends = jnp.concatenate([xtail[d].astype(jnp.float32) for d in range(n)], axis=0)
    sq_send[...] = jnp.broadcast_to(ends[:, 0:1] + ends[:, 1:2], sq_send.shape)
    sq_copy = remote(sq_send, sq_in, s_ss.at[1], s_rs.at[1], partner)
    sq_copy.start()
    def last_term(p):
        cols = slice(p * part_units, (p + 1) * part_units)
        return uown[:, cols] + jnp.dot(
            xall[...], wup_v[up_chunks - 1, :, cols], preferred_element_type=jnp.float32
        )

    ready = last_term(0)
    for p in range(parts):
        after = last_term(p + 1) if p + 1 < parts else None
        uown[:, p * part_units : (p + 1) * part_units] = ready
        usend[p] = ready.astype(jnp.bfloat16)
        exchange(p).start()
        ready = after

    sq_copy.wait_recv()
    scale = lax.rsqrt((sq_send[...] + sq_in[...])[:, 0:1] / width + eps)

    def activate(p):
        cols = slice(p * part_units, (p + 1) * part_units)
        up = (uown[:, cols] + uin[p].astype(jnp.float32)) * scale
        active[:, cols] = (up / (1.0 + jnp.exp(-up))).astype(jnp.bfloat16)

    def send_back(c, down):
        for d in range(n):
            rsend[c, d] = down[d * cap : (d + 1) * cap].astype(jnp.bfloat16)
        for step in range(n - 1):
            to = other(step)
            remote(
                rsend.at[c, to], rin.at[c, me], r_ss.at[0], r_rs.at[c], (group, to, core)
            ).start()
        rin[c, me] = rsend[c, me]

    first = min(2, down_chunks)
    downs = [None] * first
    for p in range(parts - 1):
        exchange(p).wait_recv()
    for p in range(parts):
        if p == parts - 1:
            exchange(p).wait_recv()
        activate(p)
        span = slice(p * part_units, (p + 1) * part_units)
        for c in range(first):
            if p == 0:
                down_copy(c).wait()
            term = jnp.dot(active[:, span], wdn_v[c, span], preferred_element_type=jnp.float32)
            downs[c] = term if p == 0 else downs[c] + term
    for c in range(first):
        send_back(c, downs[c])
    for c in range(first, down_chunks):
        down_copy(c).wait()
        send_back(c, jnp.dot(active[...], wdn_v[c], preferred_element_type=jnp.float32))

    stat_copy.wait_recv()
    both = small_send[0] + small_in[0]
    norm_scale = lax.rsqrt(both[:, experts : experts + 1] / width + eps)
    logits = both * norm_scale
    picked0 = jnp.sum(jnp.where(lane == route0, logits, 0.0), axis=1, keepdims=True)
    picked1 = jnp.sum(jnp.where(lane == route1, logits, 0.0), axis=1, keepdims=True)
    gate0 = 1.0 / (1.0 + jnp.exp(picked1 - picked0))
    gate1 = 1.0 / (1.0 + jnp.exp(picked0 - picked1))

    sq_part = jnp.zeros((rows, 1), jnp.float32)
    dot_part = jnp.zeros((rows, 1), jnp.float32)
    for c in range(down_chunks):
        arrival(rin.at[c, others], r_rs.at[c]).wait_recv()
        pieces = jnp.concatenate([rin[c, d].astype(jnp.float32) for d in range(n)], axis=0)
        fetched = jnp.dot(fetch, pieces.astype(jnp.bfloat16), preferred_element_type=jnp.float32)
        cols = slice(c * down_cols, (c + 1) * down_cols)
        final = hid[:, cols] + (gate0 * fetched[:rows] + gate1 * fetched[rows:])
        out_ref[:, cols] = final.astype(jnp.bfloat16)
        sq_part = sq_part + jnp.sum(final * final, axis=1, keepdims=True)
        dot_part = dot_part + jnp.sum(
            final * (fgain_ref[:, cols] * vw_ref[:, cols]), axis=1, keepdims=True
        )
    small_send[1] = jnp.where(lane == 0, sq_part, jnp.where(lane == 1, dot_part, 0.0))
    last = remote(small_send.at[1], small_in.at[1], s_ss.at[2], s_rs.at[2], partner)
    last.start()

    def sent(block, send_sem):
        remote(block, block, send_sem, r_rs.at[0], partner).wait_send()

    for step in range(1, n):

        @pl.when(me + step < n)
        def _(step=step):
            kv_copy(me, step, me).wait_send()

    sent(xin.at[:, others], x_ss.at[0])
    sent(xtail.at[others], t_ss.at[0])
    sent(rin.at[:, others], r_ss.at[0])
    for p in range(parts):
        exchange(p).wait_send()
    stat_copy.wait_send()
    sq_copy.wait_send()
    last.wait_recv()
    ends = small_send[1] + small_in[1]
    estimate = ends[:, 1:2] * lax.rsqrt(ends[:, 0:1] / width + eps) + bias_ref[0]
    place = me * rows + lax.broadcasted_iota(jnp.int32, (rows, 1), 0)
    estimate = jnp.where(place < len_ref[0], estimate, 0.0)
    val_ref[...] = jnp.sum(jnp.where(later == sooner, estimate, 0.0), axis=0, keepdims=True)
    last.wait_send()


def store_kernel(out_ref, val_ref, out_hbm, val_hbm, sem):
    copies = [
        pltpu.make_async_copy(out_ref, out_hbm, sem.at[0]),
        pltpu.make_async_copy(val_ref, val_hbm, sem.at[1]),
    ]
    for copy in copies:
        copy.start()
    for copy in copies:
        copy.wait()


def fused(
    stream,
    queries,
    key_rows,
    value_rows,
    routes,
    seq_length,
    norm_gain,
    router,
    w_up,
    w_down,
    final_gain,
    value_weight,
    value_bias,
):
    rows, half = stream.shape
    n = lax.axis_size("seq")
    experts = router.shape[1]
    hidden_units = w_up.shape[1]
    cap = rows // 2
    arrivals = n * cap
    kv_cols = key_rows.shape[1]
    up_chunks = kv_cols // HD
    up_rows = half // up_chunks
    down_cols = largest(half, 512)
    down_chunks = half // down_cols
    parts = 4
    part_units = hidden_units // parts
    vmem = pl.BlockSpec(memory_space=pltpu.VMEM)
    hbm = pl.BlockSpec(memory_space=pltpu.HBM)
    raw = pl.BlockSpec(memory_space=pl.ANY)
    bf16, f32 = jnp.bfloat16, jnp.float32
    dma = pltpu.SemaphoreType.DMA
    sem_shapes = (
        (up_chunks,),
        (down_chunks,),
        (n,),
        (n,),
        (1,),
        (up_chunks,),
        (parts,),
        (parts,),
        (1,),
        (down_chunks,),
        (3,),
        (3,),
        (1,),
        (1,),
        (11,),
    )
    out, values = pl.pallas_call(
        functools.partial(
            layer_kernel, n, experts, half * lax.axis_size("tp"), sem_shapes
        ),
        out_shape=(pltpu.VMEM((rows, half), bf16), pltpu.VMEM((1, rows), f32)),
        in_specs=[hbm] * 13,
        out_specs=(vmem, vmem),
        scratch_shapes=[
            pltpu.VMEM(stream.shape, bf16),
            pltpu.VMEM(stream.shape, bf16),
            pltpu.VMEM((2, rows), jnp.int32),
            pltpu.SMEM((1,), jnp.int32),
            pltpu.VMEM((1, half), f32),
            pltpu.VMEM((experts, half), f32),
            pltpu.VMEM((1, half), f32),
            pltpu.VMEM((1, half), f32),
            pltpu.SMEM((1,), f32),
            pltpu.VMEM((up_chunks, up_rows, hidden_units), bf16),
            pltpu.VMEM((down_chunks, hidden_units, down_cols), bf16),
            pltpu.VMEM((n, 2, rows, kv_cols), bf16),
            pltpu.VMEM((rows, half), f32),
            pltpu.VMEM((up_chunks, experts, cap, up_rows), bf16),
            pltpu.VMEM((up_chunks, n, cap, up_rows), bf16),
            pltpu.VMEM((experts, cap, LANES), bf16),
            pltpu.VMEM((n, cap, LANES), bf16),
            pltpu.VMEM((arrivals, up_rows), bf16),
            pltpu.VMEM((arrivals, hidden_units), f32),
            pltpu.VMEM((parts, arrivals, part_units), bf16),
            pltpu.VMEM((parts, arrivals, part_units), bf16),
            pltpu.VMEM((arrivals, hidden_units), bf16),
            pltpu.VMEM((down_chunks, n, cap, down_cols), bf16),
            pltpu.VMEM((down_chunks, n, cap, down_cols), bf16),
            pltpu.VMEM((2, rows, LANES), f32),
            pltpu.VMEM((2, rows, LANES), f32),
            pltpu.VMEM((arrivals, LANES), f32),
            pltpu.VMEM((arrivals, LANES), f32),
        ],
        compiler_params=pltpu.CompilerParams(
            collective_id=0,
            has_side_effects=True,
            vmem_limit_bytes=VMEM_BYTES,
        ),
        name="layer",
    )(
        stream,
        queries,
        key_rows,
        value_rows,
        routes.T,
        seq_length,
        norm_gain.reshape(1, half),
        router.T,
        w_up,
        w_down,
        final_gain.reshape(1, half),
        value_weight.reshape(1, half),
        value_bias,
    )
    out, values = pl.pallas_call(
        store_kernel,
        out_shape=(
            jax.ShapeDtypeStruct((rows, half), bf16),
            jax.ShapeDtypeStruct((1, rows), f32),
        ),
        in_specs=[raw, raw],
        out_specs=(hbm, hbm),
        scratch_shapes=[dma((2,))],
        name="store",
    )(
        pltpu.with_memory_space_constraint(out, pltpu.VMEM),
        pltpu.with_memory_space_constraint(values, pltpu.VMEM),
    )
    return out, values.reshape(rows)


def unfused(
    stream,
    queries,
    key_rows,
    value_rows,
    routes,
    seq_length,
    norm_gain,
    router,
    w_up,
    w_down,
    final_gain,
    value_weight,
    value_bias,
):
    row_count = stream.shape[0]
    half_width = stream.shape[1]
    width = half_width * lax.axis_size("tp")
    experts = router.shape[1]
    seq_devices = lax.axis_size("seq")
    owners = seq_devices // experts
    my_index = lax.axis_index("seq")
    seq_limit = seq_length[0]
    positions = my_index * row_count + jnp.arange(row_count, dtype=jnp.int32)
    kv_heads = key_rows.shape[1] // HD
    per_group = queries.shape[1] // HD // kv_heads
    grouped = queries.reshape(row_count, kv_heads, per_group, HD)
    inv_root = 1.0 / math.sqrt(HD)
    slot_cap = row_count // 2
    run_max = jnp.full((kv_heads, per_group, row_count), masked, jnp.float32)
    key_block = lax.all_gather(key_rows, "seq", axis=0, tiled=True)
    value_block = lax.all_gather(value_rows, "seq", axis=0, tiled=True)
    key_count = key_block.shape[0]
    scores = (
        jnp.einsum(
            "qkgd,ckd->kgqc",
            grouped,
            key_block.reshape(key_count, kv_heads, HD),
            preferred_element_type=jnp.float32,
        )
        * inv_root
    )
    key_pos = jnp.arange(key_count, dtype=jnp.int32)
    allowed = (key_pos[None, :] <= positions[:, None]) & (key_pos[None, :] < seq_limit)
    scores = jnp.where(allowed, scores, masked)
    new_max = jnp.maximum(run_max, jnp.max(scores, axis=-1))
    weights = jnp.where(allowed, jnp.exp(scores - new_max[..., None]), 0.0)
    new_sum = jnp.sum(weights, axis=-1)
    update = jnp.einsum(
        "kgqc,ckd->kgqd",
        weights.astype(jnp.bfloat16),
        value_block.reshape(key_count, kv_heads, HD),
        preferred_element_type=jnp.float32,
    )
    attended = (update / new_sum[..., None]).transpose(2, 0, 1, 3).reshape(row_count, half_width)
    hidden = stream.astype(jnp.float32) + attended
    gained = hidden * norm_gain
    squares = jnp.sum(hidden * hidden, axis=1)
    total_sq = lax.psum(squares, "tp")
    norm_scale = lax.rsqrt(total_sq / width + eps)
    normed = gained * norm_scale[:, None]
    logits = lax.psum(jnp.dot(normed, router, precision=lax.Precision.HIGHEST), "tp")
    normed_half = normed.astype(jnp.bfloat16)
    expert_ids = jnp.arange(experts, dtype=jnp.int32)
    chosen = (routes[:, :, None] == expert_ids).astype(jnp.float32)
    picked = jnp.sum(chosen * logits[:, None, :], axis=2)
    gates = jax.nn.sigmoid(picked - picked[:, ::-1])
    flat_hits = chosen.reshape(row_count * 2, experts)
    earlier = jnp.cumsum(flat_hits, axis=0) - flat_hits
    slot_index = jnp.sum(earlier * flat_hits, axis=1).astype(jnp.int32)
    target = routes.reshape(row_count * 2) * slot_cap + slot_index
    placing = (target[:, None] == jnp.arange(experts * slot_cap, dtype=jnp.int32)[None, :]).astype(
        jnp.bfloat16
    )
    doubled = jnp.repeat(normed_half, 2, axis=0)
    packed = jnp.einsum("pe,pd->ed", placing, doubled, preferred_element_type=jnp.float32).astype(
        jnp.bfloat16
    )
    outgoing = jnp.broadcast_to(
        packed.reshape(experts, 1, slot_cap, half_width), (experts, owners, slot_cap, half_width)
    ).reshape(seq_devices, slot_cap, half_width)
    arrived = lax.all_to_all(outgoing, "seq", split_axis=0, concat_axis=0, tiled=True)
    lead = arrived.shape[0]
    items = arrived.shape[1]
    flat_rows = arrived.reshape(lead * items, half_width)
    up_part = jnp.dot(flat_rows, w_up, preferred_element_type=jnp.float32)
    up_total = lax.psum(up_part.astype(jnp.bfloat16), "tp").astype(jnp.float32)
    active = jax.nn.silu(up_total).astype(jnp.bfloat16)
    down_part = jnp.dot(active, w_down, preferred_element_type=jnp.float32).astype(jnp.bfloat16)
    partial_out = down_part.reshape(lead, items, half_width)
    returned = lax.all_to_all(partial_out, "seq", split_axis=0, concat_axis=0, tiled=True)
    summed = jnp.sum(
        returned.reshape(experts, owners, slot_cap, half_width), axis=1, dtype=jnp.float32
    ).reshape(experts * slot_cap, half_width)
    fetched = jnp.dot(placing.astype(jnp.float32), summed, precision=lax.Precision.HIGHEST)
    mixed = jnp.sum(fetched.reshape(row_count, 2, half_width) * gates[:, :, None], axis=1)
    final = hidden + mixed
    sq_part = jnp.sum(final * final, axis=1)
    dot_part = jnp.sum(final * (final_gain * value_weight), axis=1)
    sq_total, dot_total = lax.psum((sq_part, dot_part), "tp")
    estimate = dot_total * lax.rsqrt(sq_total / width + eps) + value_bias[0]
    estimate = jnp.where(positions < seq_limit, estimate, 0.0)
    return (final.astype(jnp.bfloat16), estimate)


def on_device(*args):
    stream, w_up = args[0], args[8]
    arrivals = lax.axis_size("seq") * (stream.shape[0] // 2)
    weight_bytes = 4 * w_up.shape[0] * w_up.shape[1]
    small = arrivals <= ROW_LIMIT and weight_bytes <= 52 * 1024 * 1024
    return fused(*args) if small else unfused(*args)


def solution(mesh):
    return jax.shard_map(
        on_device,
        mesh=mesh,
        in_specs=(
            P(("groups", "seq"), "tp"),
            P(("groups", "seq"), "tp"),
            P(("groups", "seq"), "tp"),
            P(("groups", "seq"), "tp"),
            P(("groups", "seq"), None),
            P("groups"),
            P("tp"),
            P("tp", None),
            P("tp", "seq"),
            P("seq", "tp"),
            P("tp"),
            P("tp"),
            P(),
        ),
        out_specs=(P(("groups", "seq"), "tp"), P(("groups", "seq"))),
        check_vma=False,
    )
```
